16 devices in a mesh: row: 4 (over z, y), col: 4 (over x, core).
Axes of the slice: x: 2, y: 2, z: 2, core: 2. Of those that a mesh axis runs over, the one named last changes fastest.
Arguments:
- v_panels: float32 [8192, 8192], P('row', 'col')
- t_factors: float32 [128, 64, 64], P('col')
- z_vectors: float32 [8192, 2048], P(None, ('col', 'row'))
Outputs:
- output: float32 [8192, 2048], P('row', 'col')
All inputs are finite; a program needn't handle non-finite values.
Results may differ from the reference program's by a relative error of at most 0.001.
Values sent between devices are 32-bit elements.
A program may use at most 1 GiB of HBM per device.

```python
import jax
import jax.numpy as jnp
from jax import lax

MAT_ORDER = 8192
PANEL_WIDTH = 64
ROW_DEVS = 4
COL_DEVS = 4
COLS_DEV = 128
NUM_PANELS = MAT_ORDER // PANEL_WIDTH
NUM_COLS = COLS_DEV * ROW_DEVS * COL_DEVS
HIGHEST = lax.Precision.HIGHEST


def compact_factors(panels):
    gram_mat = jnp.einsum('nja,njc->jac', panels, panels, precision=HIGHEST)
    diag_half = 0.5 * gram_mat * jnp.eye(PANEL_WIDTH, dtype=jnp.float32)
    upper_mat = jnp.triu(gram_mat, 1) + diag_half
    return jnp.triu(jnp.linalg.inv(upper_mat))


def to_stored(v_log):
    rows_perm = v_log.reshape(NUM_PANELS // ROW_DEVS, ROW_DEVS, PANEL_WIDTH, MAT_ORDER)
    rows_perm = rows_perm.transpose(1, 0, 2, 3).reshape(MAT_ORDER, NUM_PANELS // COL_DEVS, COL_DEVS, PANEL_WIDTH)
    return rows_perm.transpose(0, 2, 1, 3).reshape(MAT_ORDER, MAT_ORDER)


def setup_inputs(seed: int = 0) -> dict:
    root_key = jax.random.key(seed)
    key_v, key_z = jax.random.split(root_key)
    below_diag = jax.random.normal(key_v, (MAT_ORDER, MAT_ORDER), jnp.float32)
    v_log = jnp.tril(below_diag, -1) + jnp.eye(MAT_ORDER, dtype=jnp.float32)
    t_log = compact_factors(v_log.reshape(MAT_ORDER, NUM_PANELS, PANEL_WIDTH))
    t_st = t_log.reshape(NUM_PANELS // COL_DEVS, COL_DEVS, PANEL_WIDTH, PANEL_WIDTH)
    t_st = t_st.transpose(1, 0, 2, 3).reshape(NUM_PANELS, PANEL_WIDTH, PANEL_WIDTH)
    z_draw = jax.random.normal(key_z, (MAT_ORDER, NUM_COLS), jnp.float32)
    return {'v_panels': to_stored(v_log), 't_factors': t_st, 'z_vectors': z_draw}


def reference(v_panels, t_factors, z_vectors):
    panels = v_panels.reshape(MAT_ORDER, COL_DEVS, NUM_PANELS // COL_DEVS, PANEL_WIDTH)
    panels = panels.transpose(2, 1, 0, 3).reshape(NUM_PANELS, MAT_ORDER, PANEL_WIDTH)
    factors = t_factors.reshape(COL_DEVS, NUM_PANELS // COL_DEVS, PANEL_WIDTH, PANEL_WIDTH)
    factors = factors.transpose(1, 0, 2, 3).reshape(NUM_PANELS, PANEL_WIDTH, PANEL_WIDTH)

    def apply_panel(x_cur, panel_item):
        v_j, t_j = panel_item
        w_mat = jnp.dot(v_j.T, x_cur, precision=HIGHEST, preferred_element_type=jnp.float32)
        y_mat = jnp.dot(t_j, w_mat, precision=HIGHEST, preferred_element_type=jnp.float32)
        x_new = x_cur - jnp.dot(v_j, y_mat, precision=HIGHEST, preferred_element_type=jnp.float32)
        return x_new, None

    return lax.scan(apply_panel, z_vectors, (panels, factors), reverse=True)[0]
```

```python
import jax
import jax.numpy as jnp
from jax import lax
from jax.experimental import pallas as pl
from jax.experimental.pallas import tpu as pltpu
from jax.sharding import PartitionSpec as P

F32 = jnp.float32
BF16 = jnp.bfloat16
MESH = pl.DeviceIdType.MESH
NBLK = 16
AHEAD = 4
NT = (((1,), (1,)), ((), ()))
NN = (((1,), (0,)), ((), ()))


def split3(val):
    high = val.astype(BF16)
    rest = val - high.astype(F32)
    mid = rest.astype(BF16)
    low = (rest - mid.astype(F32)).astype(BF16)
    return high, mid, low


def stack3(val):
    return jnp.concatenate(split3(val), axis=0)


def dot6(stack, b_high, b_mid, b_low, dims):
    rows = stack.shape[0] // 3
    o_high = lax.dot_general(stack, b_high, dims, preferred_element_type=F32)
    o_mid = lax.dot_general(stack[:2 * rows], b_mid, dims, preferred_element_type=F32)
    o_low = lax.dot_general(stack[:rows], b_low, dims, preferred_element_type=F32)
    small = (o_high[2 * rows:] + o_mid[rows:]) + o_low
    return o_high[:rows] + ((o_high[rows:2 * rows] + o_mid[:rows]) + small)


def kernel(v, tt, z4, o, vb, zb, vp, xt, stage, zst, tbv, ts, tp, ys, wsend, wrecv, gsend, grecv, osb,
           v_s, v_r, z_s, z_r, zl, tb_s, tb_r, tb_l, t_s, t_r, w_s, w_r, g_s, g_r, st_a, st_b, o_s, o_r, o_l):
    r = lax.axis_index('row')
    c = lax.axis_index('col')
    zz, yy, xx, kk = r // 2, r % 2, c // 2, c % 2
    dev_x = (r, (1 - xx) * 2 + kk)
    dev_y = (zz * 2 + (1 - yy), c)
    dev_z = ((1 - zz) * 2 + yy, c)
    dev_p = (r, xx * 2 + (1 - kk))
    dev_d = (zz * 2 + yy + (1 - kk) * (1 - 2 * yy), (xx + kk * (1 - 2 * xx)) * 2 + kk)

    barrier = pltpu.get_barrier_semaphore()
    for dev in (dev_x, dev_y, dev_z, dev_p):
        pl.semaphore_signal(barrier, 1, device_id=dev, device_id_type=MESH)
    pl.semaphore_wait(barrier, 4)

    def remote(src, dst, s_sem, r_sem, dev):
        return pltpu.make_async_remote_copy(src_ref=src, dst_ref=dst, send_sem=s_sem, recv_sem=r_sem,
                                            device_id=dev, device_id_type=MESH)

    def own(qq, idx, dev):
        r0 = 128 * qq
        return remote(v.at[pl.ds(r0, 2048 - r0), pl.ds(r0, 128)], vb.at[qq, idx, pl.ds(r0, 2048 - r0)],
                      v_s.at[qq, idx], v_r.at[qq, idx], dev)

    def fwd(qq, src, idx, dev):
        r0 = 128 * qq
        return remote(vb.at[qq, src, pl.ds(r0, 2048 - r0)], vb.at[qq, idx, pl.ds(r0, 2048 - r0)],
                      v_s.at[qq, idx], v_r.at[qq, idx], dev)

    def slab(qq, idx):
        if idx in (0, 1, 3):
            return own(qq, idx, {0: dev_p, 1: dev_x, 3: dev_y}[idx])
        if idx == 5:
            return fwd(qq, 1 + 2 * kk, 5, dev_d)
        return fwd(qq, idx - 1, idx, dev_p)

    def at_q(q, fn):
        for qq in range(NBLK):
            @pl.when(q == qq)
            def _():
                fn(qq)

    def send_own(qq):
        for idx in (1, 3, 0):
            slab(qq, idx).start()

    def pass_on(qq):
        for idx in (1, 3):
            slab(qq, idx).wait_recv()
        for idx in (5, 2, 4):
            slab(qq, idx).start()

    def pass_diag(qq):
        slab(qq, 5).wait_recv()
        slab(qq, 6).start()

    def all_here(qq):
        for idx in (0, 2, 4, 6):
            slab(qq, idx).wait_recv()

    def z_copy(ch):
        rows = pl.ds(pl.multiple_of(256 * ch, 256), 256)
        return remote(z4.at[pl.ds(2 * (1 - zz), 2), rows], zb.at[:, rows], z_s.at[ch], z_r.at[ch], dev_z)

    def z_loads(ch):
        rows = pl.ds(pl.multiple_of(256 * ch, 256), 256)
        return (pltpu.make_async_copy(z4.at[pl.ds(2 * zz, 2), rows], zst.at[zz], zl.at[0]),
                pltpu.make_async_copy(zb.at[:, rows], zst.at[1 - zz], zl.at[1]))

    halves = ((12, 4), (0, 12))

    def t_copy(half, way):
        q0, nq = halves[half]
        part = pl.ds(q0, nq)
        src = tbv.at[2, part] if way == 2 else tt.at[part]
        return remote(src, tbv.at[way + 1, part], tb_s.at[half, way], tb_r.at[half, way],
                      dev_x if way == 1 else dev_p)

    def w_copy(s, par):
        return remote(wsend.at[s, par], wrecv.at[s, par], w_s.at[s, par], w_r.at[s, par], dev_z)

    def g_copy(slot):
        return remote(gsend.at[slot], grecv.at[slot], g_s.at[slot], g_r.at[slot], dev_z)

    def s_copy(slot):
        return remote(ts.at[slot, kk], ts.at[slot, kk], t_s.at[slot], t_r.at[slot], dev_p)

    own_t = pltpu.make_async_copy(tt, tbv.at[0], tb_l)
    own_t.start()
    for way in range(2):
        t_copy(0, way).start()
    send_own(15)
    z_copy(7).start()
    send_own(14)
    z_copy(6).start()
    send_own(13)
    for way in range(2):
        t_copy(1, way).start()
    own_t.wait()

    lane = lax.broadcasted_iota(jnp.int32, (128, 128), 1)
    left = lane < 64
    left64 = left[:64]

    def stage_loads(q, ch, buf):
        rows = pl.ds(pl.multiple_of(256 * ch, 256), 256)
        cols = pl.ds(pl.multiple_of(128 * q, 128), 128)
        return (pltpu.make_async_copy(v.at[rows, cols], stage.at[buf, 0], st_a.at[buf]),
                pltpu.make_async_copy(vb.at[q, :, rows], stage.at[buf, pl.ds(1, 7)], st_b.at[buf]))

    def prepare(qn, slot):
        cq = qn // 2
        n = 8 - cq
        gsend[slot] = jnp.zeros((192, 256), F32)
        for cp in stage_loads(qn, 7, 0):
            cp.start()

        def chunk(j, _):
            ch = 7 - j
            buf = j % 2

            @pl.when(j + 1 < n)
            def _():
                for cp in stage_loads(qn, ch - 1, 1 - buf):
                    cp.start()

            for cp in stage_loads(qn, ch, buf):
                cp.wait()
            empty = (qn % 2 == 1) & (ch == cq)
            for y1 in range(2):
                dy = (y1 + yy) % 2
                for h in range(2):
                    for pair in range(2):
                        dx = (pair + xx) % 2
                        rel = dy * 4 + dx * 2
                        a0 = stage[buf, rel + kk, pl.ds(128 * h, 128), :]
                        a1 = stage[buf, rel + 1 - kk, pl.ds(128 * h, 128), :]
                        if h == 0:
                            a0 = jnp.where(empty, 0.0, a0)
                            a1 = jnp.where(empty, 0.0, a1)
                        r0 = pltpu.roll(a0, 64, 1)
                        r1 = pltpu.roll(a1, 64, 1)
                        vals = (jnp.where(left, a0, r1), jnp.where(left, r0, a1))
                        for par in range(2):
                            parts = split3(vals[par])
                            for piece in range(3):
                                vp[slot, par, piece, ch, pl.ds(y1 * 256 + h * 128, 128),
                                   pl.ds(pair * 128, 128)] = parts[piece]
            vh = vp[slot, kk, 0, ch]
            vm = vp[slot, kk, 1, ch]
            vl = vp[slot, kk, 2, ch]
            lhs = jnp.concatenate([vh.T[64:], vm.T[64:], vl.T[64:]], axis=0)
            gsend[slot] += dot6(lhs, vh, vm, vl, NN)
            return 0

        lax.fori_loop(0, n, chunk, 0)

    def form_t(qn, slot):
        zero = jnp.zeros((64, 128), F32)
        rows = []
        for e in range(4):
            dx = (e // 2 + xx) % 2
            dk = (e % 2 + kk) % 2
            val = tbv[dx * 2 + dk, qn]
            other = pltpu.roll(val, 64, 1)
            if e % 2 == 0:
                piece = jnp.where(left64, jnp.where(kk == 0, val, other), 0.0)
            else:
                piece = jnp.where(left64, 0.0, jnp.where(kk == 0, other, val))
            rows.append(jnp.concatenate([piece, zero] if e < 2 else [zero, piece], axis=1))
        s0 = jnp.concatenate(rows, axis=0)
        gram = jnp.concatenate([jnp.zeros((64, 256), F32), gsend[slot] + grecv[slot]], axis=0)
        bi = lax.broadcasted_iota(jnp.int32, (256, 256), 0) // 64
        bj = lax.broadcasted_iota(jnp.int32, (256, 256), 1) // 64
        near = ((bi == 1) & (bj == 0)) | ((bi == 3) & (bj == 2))
        far = (bi >= 2) & (bj < 2)
        for mask in (near, far):
            gm = split3(jnp.where(mask, gram, 0.0))
            sp = split3(s0)
            st = jnp.concatenate(sp, axis=0)
            mid = dot6(st, *gm, NN)
            s0 = s0 - dot6(stack3(mid), *sp, NN)
        ts[slot, kk] = s0

    def update(s, slot, par, ch):
        yst = ys[...]
        delta = dot6(yst, vp[slot, par, 0, ch], vp[slot, par, 1, ch], vp[slot, par, 2, ch], NT)
        new = xt[s, ch] - delta
        xt[s, ch] = new
        return new

    def project(s, slot, par, ch, into):
        wsend[s, into] += dot6(stack3(xt[s, ch]), vp[slot, par, 0, ch], vp[slot, par, 1, ch], vp[slot, par, 2, ch], NN)

    def out_copies(s, ch):
        rows = pl.ds(pl.multiple_of(256 * ch, 256), 256)
        cols = pl.ds(pl.multiple_of((2 * s + yy) * 128, 128), 128)
        return (pltpu.make_async_copy(osb.at[s, ch, yy], o.at[rows, cols], o_l.at[s, ch]),
                remote(osb.at[s, ch, 1 - yy], o.at[rows, cols], o_s.at[s, ch], o_r.at[s, ch], dev_y))

    def step(g, _):
        i = g // 4 - 1
        sub = g % 4
        q = 15 - i
        qn = 14 - i
        par = 1 - sub // 2
        s = sub % 2
        cur = (i + 2) % 2
        nxt = (i + 1) % 2
        more = i < 15

        @pl.when((sub == 0) & more)
        def _():
            at_q(qn, pass_on)

            @pl.when(i + AHEAD < NBLK)
            def _():
                at_q(15 - (i + AHEAD), send_own)

            @pl.when(qn % 2 == 1)
            def _():
                ch = qn // 2

                @pl.when(ch >= 2)
                def _():
                    z_copy(ch - 2).start()
                z_copy(ch).wait_recv()
                for cp in z_loads(ch):
                    cp.start()

        @pl.when(g == 0)
        def _():
            t_copy(0, 1).wait_recv()
            t_copy(0, 2).start()

        @pl.when(g == 3)
        def _():
            t_copy(0, 0).wait_recv()
            t_copy(0, 2).wait_recv()

        @pl.when(g == 5)
        def _():
            t_copy(1, 1).wait_recv()
            t_copy(1, 2).start()

        @pl.when(g == 9)
        def _():
            t_copy(1, 0).wait_recv()
            t_copy(1, 2).wait_recv()

        @pl.when((sub == 0) & (i >= 0))
        def _():
            s_copy(cur).wait()
            for pp in range(2):
                for piece, val in enumerate(split3(ts[cur, pp])):
                    tp[pp, piece] = val

        @pl.when((sub == 1) & more)
        def _():
            at_q(qn, pass_diag)

        @pl.when((sub == 2) & more)
        def _():
            at_q(qn, all_here)
            prepare(qn, nxt)
            g_copy(nxt).start()

            @pl.when(qn % 2 == 1)
            def _():
                ch = qn // 2
                for cp in z_loads(ch):
                    cp.wait()
                for ss in range(2):
                    for y1 in range(2):
                        xt[ss, ch, :, pl.ds(y1 * 256, 256)] = zst[ss, y1].T

        @pl.when((sub == 3) & more)
        def _():
            g_copy(nxt).wait()
            form_t(qn, nxt)
            s_copy(nxt).start()

        has_u = i >= 0
        has_w = ((i < 15) | (sub < 2)) & ((i >= 0) | (sub >= 2))
        n = 8 - q // 2
        w_par = 1 - par
        w_slot = jnp.where(sub < 2, cur, nxt)
        n_w = jnp.where(sub < 2, n, 8 - qn // 2)

        @pl.when(has_u)
        def _():
            w_copy(s, par).wait()
            w_sum = wsend[s, par] + wrecv[s, par]
            y_val = dot6(stack3(w_sum), tp[par, 0], tp[par, 1], tp[par, 2], NN)
            ys[...] = stack3(y_val)

        @pl.when(has_w)
        def _():
            wsend[s, w_par] = jnp.zeros((128, 256), F32)

        @pl.when(has_u & has_w)
        def _():
            update(s, cur, par, 7)

            def both(j, _):
                update(s, cur, par, 7 - j)
                project(s, w_slot, w_par, 8 - j, w_par)
                return 0
            lax.fori_loop(1, n, both, 0)

        @pl.when(has_w)
        def _():
            def rest(j, _):
                project(s, w_slot, w_par, 7 - j, w_par)
                return 0
            lax.fori_loop(jnp.where(has_u, n - 1, 0), n_w, rest, 0)
            w_copy(s, w_par).start()

        @pl.when(has_u & jnp.logical_not(has_w))
        def _():
            def last(j, _):
                ch = 7 - j
                new = update(s, cur, par, ch)
                for y1 in range(2):
                    osb[s, ch, y1] = new[:, y1 * 256:(y1 + 1) * 256].T
                for cp in out_copies(s, ch):
                    cp.start()
                return 0
            lax.fori_loop(0, 8, last, 0)
        return 0

    lax.fori_loop(0, 4 * (NBLK + 1), step, 0)

    for half in range(2):
        for way in range(3):
            t_copy(half, way).wait_send()
    for qq in range(NBLK):
        for idx in range(7):
            slab(qq, idx).wait_send()

    def drain(ch, _):
        z_copy(ch).wait_send()
        for s in range(2):
            local, far = out_copies(s, ch)
            local.wait()
            far.wait()
        return 0
    lax.fori_loop(0, 8, drain, 0)


def solution(mesh):
    def local_apply(v_loc, t_loc, z_loc):
        tt = jnp.swapaxes(t_loc, 1, 2).reshape(NBLK, 2, 64, 64).transpose(0, 2, 1, 3).reshape(NBLK, 64, 128)
        z4 = z_loc.reshape(4, 2048, 128)
        any_spec = pl.BlockSpec(memory_space=pl.ANY)
        dma, vmem = pltpu.SemaphoreType.DMA, pltpu.VMEM
        out = pl.pallas_call(
            kernel,
            out_shape=(jax.ShapeDtypeStruct((2048, 512), F32),
                       jax.ShapeDtypeStruct((NBLK, 7, 2048, 128), F32),
                       jax.ShapeDtypeStruct((2, 2048, 128), F32)),
            in_specs=[any_spec] * 3,
            out_specs=(any_spec,) * 3,
            scratch_shapes=[
                vmem((2, 2, 3, 8, 512, 256), BF16),
                vmem((2, 8, 128, 512), F32),
                vmem((2, 8, 256, 128), F32),
                vmem((2, 2, 256, 128), F32),
                vmem((4, NBLK, 64, 128), F32),
                vmem((2, 2, 256, 256), F32),
                vmem((2, 3, 256, 256), BF16),
                vmem((384, 256), BF16),
                vmem((2, 2, 128, 256), F32),
                vmem((2, 2, 128, 256), F32),
                vmem((2, 192, 256), F32),
                vmem((2, 192, 256), F32),
                vmem((2, 8, 2, 256, 128), F32),
                dma((NBLK, 7)), dma((NBLK, 7)),
                dma((8,)), dma((8,)), dma((2,)),
                dma((2, 3)), dma((2, 3)), dma,
                dma((2,)), dma((2,)),
                dma((2, 2)), dma((2, 2)),
                dma((2,)), dma((2,)),
                dma((2,)), dma((2,)),
                dma((2, 8)), dma((2, 8)), dma((2, 8)),
            ],
            compiler_params=pltpu.CompilerParams(collective_id=0, has_side_effects=True, vmem_limit_bytes=64_000_000),
        )(v_loc, tt, z4)
        return out[0]

    return jax.shard_map(local_apply, mesh=mesh,
                         in_specs=(P('row', 'col'), P('col', None, None), P(None, ('col', 'row'))),
                         out_specs=P('row', 'col'), check_vma=False)
```

```python
import jax
import jax.numpy as jnp
from jax import lax
from jax.experimental import pallas as pl
from jax.experimental.pallas import tpu as pltpu
from jax.sharding import PartitionSpec as P

F32 = jnp.float32
BF16 = jnp.bfloat16
MESH = pl.DeviceIdType.MESH
NBLK = 16
NT = (((1,), (1,)), ((), ()))
NN = (((1,), (0,)), ((), ()))


def split3(val):
    high = val.astype(BF16)
    rest = val - high.astype(F32)
    mid = rest.astype(BF16)
    low = (rest - mid.astype(F32)).astype(BF16)
    return high, mid, low


def stack3(val):
    return jnp.concatenate(split3(val), axis=0)


def dot6(stack, b_high, b_mid, b_low, dims):
    rows = stack.shape[0] // 3
    o_high = lax.dot_general(stack, b_high, dims, preferred_element_type=F32)
    o_mid = lax.dot_general(stack[:2 * rows], b_mid, dims, preferred_element_type=F32)
    o_low = lax.dot_general(stack[:rows], b_low, dims, preferred_element_type=F32)
    small = (o_high[2 * rows:] + o_mid[rows:]) + o_low
    return o_high[:rows] + ((o_high[rows:2 * rows] + o_mid[:rows]) + small)


def v_table():
    table = {}

    def add(trip, quarter, what, blk):
        if 0 <= blk < NBLK:
            table.setdefault((trip, quarter), []).append((what, blk))

    for trip in range(-1, NBLK):
        if trip >= 0:
            add(trip, 0, 'fwd', trip + 4)
            add(trip, 2, 'diag', trip + 3)
        add(trip, 0, 'own', trip + 6)
        add(trip, 3, 'here', trip + 2)
    for quarter, what, blk in ((1, 'fwd', 2), (1, 'diag', 1), (2, 'fwd', 3), (3, 'diag', 2)):
        table.setdefault((-1, quarter), []).insert(0, (what, blk))
    return table


def kernel(v, tt, z4, o, vb, zb, vp, xt, stage, zst, tbv, ts, tp, ys, wsend, wrecv, gacc, gsend, grecv, osb,
           v_s, v_r, z_s, z_r, zl, tb_s, tb_r, tb_l, t_s, t_r, w_s, w_r, g_s, g_r, st_a, st_b, o_s, o_r, o_l):
    r = lax.axis_index('row')
    c = lax.axis_index('col')
    zz, yy, xx, kk = r // 2, r % 2, c // 2, c % 2
    dev_x = (r, (1 - xx) * 2 + kk)
    dev_y = (zz * 2 + (1 - yy), c)
    dev_z = ((1 - zz) * 2 + yy, c)
    dev_p = (r, xx * 2 + (1 - kk))
    dev_d = (zz * 2 + yy + (1 - kk) * (1 - 2 * yy), (xx + kk * (1 - 2 * xx)) * 2 + kk)

    barrier = pltpu.get_barrier_semaphore()
    for dev in (dev_x, dev_y, dev_z, dev_p):
        pl.semaphore_signal(barrier, 1, device_id=dev, device_id_type=MESH)
    pl.semaphore_wait(barrier, 4)

    def remote(src, dst, s_sem, r_sem, dev):
        return pltpu.make_async_remote_copy(src_ref=src, dst_ref=dst, send_sem=s_sem, recv_sem=r_sem,
                                            device_id=dev, device_id_type=MESH)

    def mult(val, by):
        return val if isinstance(val, int) else pl.multiple_of(val, by)

    def own(qq, idx, dev):
        r0 = 128 * qq
        return remote(v.at[pl.ds(r0, 2048 - r0), pl.ds(r0, 128)], vb.at[qq, idx, pl.ds(r0, 2048 - r0)],
                      v_s.at[qq, idx], v_r.at[qq, idx], dev)

    def fwd(qq, src, idx, dev):
        r0 = 128 * qq
        return remote(vb.at[qq, src, pl.ds(r0, 2048 - r0)], vb.at[qq, idx, pl.ds(r0, 2048 - r0)],
                      v_s.at[qq, idx], v_r.at[qq, idx], dev)

    def slab(qq, idx):
        if idx in (0, 1, 3):
            return own(qq, idx, {0: dev_p, 1: dev_x, 3: dev_y}[idx])
        if idx == 5:
            return fwd(qq, 1 + 2 * kk, 5, dev_d)
        return fwd(qq, idx - 1, idx, dev_p)

    def at_trip(i, table):
        for first in range(-1, NBLK, 4):
            mine = [t for t in range(first, first + 4) if t in table]
            if mine:
                @pl.when((i >= first) & (i < first + 4))
                def _():
                    for trip in mine:
                        @pl.when(i == trip)
                        def _():
                            table[trip]()

    def send_own(qq):
        for idx in (1, 3, 0):
            slab(qq, idx).start()

    def pass_on(qq):
        for idx in (1, 3):
            slab(qq, idx).wait_recv()
        for idx in (5, 2, 4):
            slab(qq, idx).start()

    def pass_diag(qq):
        slab(qq, 5).wait_recv()
        slab(qq, 6).start()

    def stage_loads(q, ch, buf):
        rows = pl.ds(mult(256 * ch, 256), 256)
        cols = pl.ds(mult(128 * q, 128), 128)
        return (pltpu.make_async_copy(v.at[rows, cols], stage.at[buf, 0], st_a.at[buf]),
                pltpu.make_async_copy(vb.at[q, :, rows], stage.at[buf, pl.ds(1, 7)], st_b.at[buf]))

    def all_here(qq):
        for idx in (0, 2, 4, 6):
            slab(qq, idx).wait_recv()
        for j in range(min(2, 8 - qq // 2)):
            for cp in stage_loads(qq, 7 - j, j):
                cp.start()

    do = {'own': send_own, 'fwd': pass_on, 'diag': pass_diag, 'here': all_here}

    def run_of(events):
        def run():
            for what, blk in events:
                do[what](15 - blk)
        return run

    def z_copy(ch):
        rows = pl.ds(pl.multiple_of(256 * ch, 256), 256)
        return remote(z4.at[pl.ds(2 * (1 - zz), 2), rows], zb.at[:, rows], z_s.at[ch], z_r.at[ch], dev_z)

    def z_loads(ch):
        rows = pl.ds(pl.multiple_of(256 * ch, 256), 256)
        return (pltpu.make_async_copy(z4.at[pl.ds(2 * zz, 2), rows], zst.at[zz], zl.at[0]),
                pltpu.make_async_copy(zb.at[:, rows], zst.at[1 - zz], zl.at[1]))

    halves = ((12, 4), (0, 12))

    def t_copy(half, way):
        q0, nq = halves[half]
        part = pl.ds(q0, nq)
        src = tbv.at[2, part] if way == 2 else tt.at[part]
        return remote(src, tbv.at[way + 1, part], tb_s.at[half, way], tb_r.at[half, way],
                      dev_x if way == 1 else dev_p)

    def w_copy(s, par):
        return remote(wsend.at[s, par], wrecv.at[s, par], w_s.at[s, par], w_r.at[s, par], dev_z)

    def g_copy(slot):
        return remote(gsend.at[slot], grecv.at[slot], g_s.at[slot], g_r.at[slot], dev_z)

    def s_copy(slot):
        return remote(ts.at[slot, kk], ts.at[slot, kk], t_s.at[slot], t_r.at[slot], dev_p)

    own_t = pltpu.make_async_copy(tt, tbv.at[0], tb_l)
    own_t.start()
    send_own(15)
    send_own(14)
    for way in range(2):
        t_copy(0, way).start()
    z_copy(7).start()
    z_copy(6).start()
    send_own(13)
    pass_on(15)
    pass_on(14)
    send_own(12)
    pass_diag(15)
    send_own(11)
    for way in range(2):
        t_copy(1, way).start()
    own_t.wait()
    all_here(15)

    lane = lax.broadcasted_iota(jnp.int32, (128, 128), 1)
    left = lane < 64
    left64 = left[:64]

    def prepare(qn, slot):
        cq = qn // 2
        n = 8 - cq
        gacc[...] = jnp.zeros((192, 256), F32)

        def take(j):
            ch = 7 - j
            buf = j % 2
            for cp in stage_loads(qn, ch, buf):
                cp.wait()

        def parts(j):
            ch = 7 - j
            buf = j % 2
            empty = (qn % 2 == 1) & (ch == cq)
            for y1 in range(2):
                dy = (y1 + yy) % 2
                for h in range(2):
                    for pair in range(2):
                        dx = (pair + xx) % 2
                        rel = dy * 4 + dx * 2
                        a0 = stage[buf, rel + kk, pl.ds(128 * h, 128), :]
                        a1 = stage[buf, rel + 1 - kk, pl.ds(128 * h, 128), :]
                        if h == 0:
                            a0 = jnp.where(empty, 0.0, a0)
                            a1 = jnp.where(empty, 0.0, a1)
                        r0 = pltpu.roll(a0, 64, 1)
                        r1 = pltpu.roll(a1, 64, 1)
                        vals = (jnp.where(left, a0, r1), jnp.where(left, r0, a1))
                        for par in range(2):
                            for piece, val in enumerate(split3(vals[par])):
                                vp[slot, par, piece, ch, pl.ds(y1 * 256 + h * 128, 128),
                                   pl.ds(pair * 128, 128)] = val

        def more_loads(j):
            @pl.when(j + 2 < n)
            def _():
                for cp in stage_loads(qn, 5 - j, j % 2):
                    cp.start()

        def gram(j):
            vh, vm, vl = (vp[slot, kk, piece, 7 - j] for piece in range(3))
            lhs = jnp.concatenate([vh.T[64:], vm.T[64:], vl.T[64:]], axis=0)
            prod = dot6(lhs, vh, vm, vl, NN)
            gacc[...] += prod

        take(0)
        parts(0)
        more_loads(0)

        def trip(j, _):
            take(j)
            gram(j - 1)
            parts(j)
            more_loads(j)
            return 0
        lax.fori_loop(1, n, trip, 0)
        gram(n - 1)
        gsend[slot, pl.ds(0, 192)] = gacc[:, pl.ds(0, 128)]
        gsend[slot, pl.ds(192, 64)] = gacc[pl.ds(128, 64), pl.ds(128, 128)]

    def form_t(qn, slot):
        zero = jnp.zeros((64, 128), F32)

        def panel(e):
            val = tbv[(e // 2 + xx) % 2 * 2 + (e % 2 + kk) % 2, qn]
            other = pltpu.roll(val, 64, 1)
            return (jnp.where(left64, jnp.where(kk == 0, val, other), 0.0),
                    jnp.where(left64, 0.0, jnp.where(kk == 0, other, val)))

        def padded(val):
            return split3(jnp.concatenate([val, zero], axis=0))

        gram = gsend[slot] + grecv[slot]
        first, second = [], []
        for pair in range(2):
            low, high = panel(2 * pair)[0], panel(2 * pair + 1)
            near = jnp.where(left64, gram[192 * pair:192 * pair + 64], 0.0)
            first.append(dot6(stack3(high[0]), *padded(near), NN))
            second.append((low, high[1]))
        pairs = []
        for pair in range(2):
            low, high = second[pair]
            pairs.append(jnp.concatenate([low, high - dot6(stack3(first[pair]), *padded(low), NN)], axis=0))
        far = dot6(stack3(pairs[1]), *split3(gram[64:192]), NN)
        far = dot6(stack3(far), *split3(pairs[0]), NN)
        ts[slot, kk, pl.ds(0, 128), pl.ds(0, 128)] = pairs[0]
        ts[slot, kk, pl.ds(0, 128), pl.ds(128, 128)] = jnp.zeros((128, 128), F32)
        ts[slot, kk, pl.ds(128, 128), pl.ds(0, 128)] = -far
        ts[slot, kk, pl.ds(128, 128), pl.ds(128, 128)] = pairs[1]

    def update(s, slot, par, ch):
        yst = ys[...]
        delta = dot6(yst, vp[slot, par, 0, ch], vp[slot, par, 1, ch], vp[slot, par, 2, ch], NT)
        new = xt[s, ch] - delta
        xt[s, ch] = new
        return new

    def project(s, slot, par, ch, into):
        wsend[s, into] += dot6(stack3(xt[s, ch]), vp[slot, par, 0, ch], vp[slot, par, 1, ch], vp[slot, par, 2, ch], NN)

    def out_copies(s, ch):
        rows = pl.ds(pl.multiple_of(256 * ch, 256), 256)
        cols = pl.ds(pl.multiple_of((2 * s + yy) * 128, 128), 128)
        return (pltpu.make_async_copy(osb.at[s, ch, yy], o.at[rows, cols], o_l.at[s, ch]),
                remote(osb.at[s, ch, 1 - yy], o.at[rows, cols], o_s.at[s, ch], o_r.at[s, ch], dev_y))

    events = v_table()

    def step(g, _):
        i = g // 4 - 1
        sub = g % 4
        q = 15 - i
        qn = 14 - i
        par = 1 - sub // 2
        s = sub % 2
        cur = (i + 2) % 2
        nxt = (i + 1) % 2
        more = i < 15

        for quarter in range(4):
            here = {trip: run_of(ev) for (trip, at), ev in events.items() if at == quarter}

            @pl.when(sub == quarter)
            def _():
                at_trip(i, here)

        @pl.when(g == 0)
        def _():
            t_copy(0, 1).wait_recv()
            t_copy(0, 2).start()

        @pl.when(g == 2)
        def _():
            t_copy(0, 0).wait_recv()
            t_copy(0, 2).wait_recv()

        @pl.when(g == 5)
        def _():
            t_copy(1, 1).wait_recv()
            t_copy(1, 2).start()

        @pl.when(g == 9)
        def _():
            t_copy(1, 0).wait_recv()
            t_copy(1, 2).wait_recv()

        @pl.when((sub == 0) & (i >= 0))
        def _():
            s_copy(cur).wait()
            for pp in range(2):
                for piece, val in enumerate(split3(ts[cur, pp])):
                    tp[pp, piece] = val

        @pl.when((sub == 0) & more)
        def _():
            prepare(qn, nxt)

        @pl.when((sub == 1) & more & (qn % 2 == 1))
        def _():
            ch = qn // 2
            z_copy(ch).wait_recv()
            for cp in z_loads(ch):
                cp.start()

        @pl.when((sub == 2) & more)
        def _():
            @pl.when(qn % 2 == 1)
            def _():
                ch = qn // 2
                for cp in z_loads(ch):
                    cp.wait()
                for ss in range(2):
                    for y1 in range(2):
                        xt[ss, ch, :, pl.ds(y1 * 256, 256)] = zst[ss, y1].T

            g_copy(nxt).wait()
            form_t(qn, nxt)
            s_copy(nxt).start()

        has_u = i >= 0
        has_w = ((i < 15) | (sub < 2)) & ((i >= 0) | (sub >= 2))
        n = 8 - q // 2
        w_par = 1 - par
        w_slot = jnp.where(sub < 2, cur, nxt)
        n_w = jnp.where(sub < 2, n, 8 - qn // 2)

        @pl.when(has_u)
        def _():
            w_copy(s, par).wait()
            w_sum = wsend[s, par] + wrecv[s, par]
            y_val = dot6(stack3(w_sum), tp[par, 0], tp[par, 1], tp[par, 2], NN)
            ys[...] = stack3(y_val)
            update(s, cur, par, 7)

        @pl.when(has_w)
        def _():
            wsend[s, w_par] = jnp.zeros((128, 256), F32)

        @pl.when(has_u & has_w)
        def _():
            def both(j, _):
                project(s, w_slot, w_par, 8 - j, w_par)
                update(s, cur, par, 7 - j)
                return 0
            lax.fori_loop(1, n, both, 0)

        @pl.when(has_w)
        def _():
            def rest(j, _):
                project(s, w_slot, w_par, 7 - j, w_par)
                return 0
            lax.fori_loop(jnp.where(has_u, n - 1, 0), n_w, rest, 0)
            w_copy(s, w_par).start()

        @pl.when((sub == 0) & more)
        def _():
            g_copy(nxt).start()

            @pl.when((qn % 2 == 1) & (qn >= 5))
            def _():
                z_copy(qn // 2 - 2).start()

        @pl.when(has_u & jnp.logical_not(has_w))
        def _():
            def give(ch):
                for y1 in range(2):
                    osb[s, ch, y1] = xt[s, ch, :, pl.ds(y1 * 256, 256)].T
                for cp in out_copies(s, ch):
                    cp.start()

            def last(j, _):
                give(8 - j)
                update(s, cur, par, 7 - j)
                return 0
            lax.fori_loop(1, 8, last, 0)
            give(0)
        return 0

    lax.fori_loop(0, 4 * (NBLK + 1), step, 0)

    for half in range(2):
        for way in range(3):
            t_copy(half, way).wait_send()
    for qq in range(NBLK):
        for idx in range(7):
            slab(qq, idx).wait_send()

    def drain(ch, _):
        z_copy(ch).wait_send()
        for s in range(2):
            local, far = out_copies(s, ch)
            local.wait()
            far.wait()
        return 0
    lax.fori_loop(0, 8, drain, 0)


def solution(mesh):
    def local_apply(v_loc, t_loc, z_loc):
        tt = jnp.swapaxes(t_loc, 1, 2).reshape(NBLK, 2, 64, 64).transpose(0, 2, 1, 3).reshape(NBLK, 64, 128)
        z4 = z_loc.reshape(4, 2048, 128)
        any_spec = pl.BlockSpec(memory_space=pl.ANY)
        dma, vmem = pltpu.SemaphoreType.DMA, pltpu.VMEM
        out = pl.pallas_call(
            kernel,
            out_shape=(jax.ShapeDtypeStruct((2048, 512), F32),
                       jax.ShapeDtypeStruct((NBLK, 7, 2048, 128), F32),
                       jax.ShapeDtypeStruct((2, 2048, 128), F32)),
            in_specs=[any_spec] * 3,
            out_specs=(any_spec,) * 3,
            scratch_shapes=[
                vmem((2, 2, 3, 8, 512, 256), BF16),
                vmem((2, 8, 128, 512), F32),
                vmem((2, 8, 256, 128), F32),
                vmem((2, 2, 256, 128), F32),
                vmem((4, NBLK, 64, 128), F32),
                vmem((2, 2, 256, 256), F32),
                vmem((2, 3, 256, 256), BF16),
                vmem((384, 256), BF16),
                vmem((2, 2, 128, 256), F32),
                vmem((2, 2, 128, 256), F32),
                vmem((192, 256), F32),
                vmem((2, 256, 128), F32),
                vmem((2, 256, 128), F32),
                vmem((2, 8, 2, 256, 128), F32),
                dma((NBLK, 7)), dma((NBLK, 7)),
                dma((8,)), dma((8,)), dma((2,)),
                dma((2, 3)), dma((2, 3)), dma,
                dma((2,)), dma((2,)),
                dma((2, 2)), dma((2, 2)),
                dma((2,)), dma((2,)),
                dma((2,)), dma((2,)),
                dma((2, 8)), dma((2, 8)), dma((2, 8)),
            ],
            compiler_params=pltpu.CompilerParams(collective_id=0, has_side_effects=True, vmem_limit_bytes=64_000_000),
        )(v_loc, tt, z4)
        return out[0]

    return jax.shard_map(local_apply, mesh=mesh,
                         in_specs=(P('row', 'col'), P('col', None, None), P(None, ('col', 'row'))),
                         out_specs=P('row', 'col'), check_vma=False)
```

```python
import jax
import jax.numpy as jnp
from jax import lax
from jax.experimental import pallas as pl
from jax.experimental.pallas import tpu as pltpu
from jax.sharding import PartitionSpec as P

F32 = jnp.float32
BF16 = jnp.bfloat16
MESH = pl.DeviceIdType.MESH
NBLK = 16
OWN = (None, None, None, 0, 3, 3, 13, 13, 3, 12, 24, 25, 34, 39, 44, 49)
FWD = (None, 3, 3, 6, 11, 8, 19, 21, 19, 21, 31, 35, 39, 46, 49, 55)
DIAG = (None, 3, 4, 10, 13, 14, 22, 25, 29, 32, 34, 41, 43, 49, 53, 57)
HERE = (None, 3, 7, 11, 15, 19, 23, 27, 31, 35, 39, 43, 47, 51, 55, 59)
NT = (((1,), (1,)), ((), ()))
NN = (((1,), (0,)), ((), ()))


def split3(val):
    high = val.astype(BF16)
    rest = val - high.astype(F32)
    mid = rest.astype(BF16)
    low = (rest - mid.astype(F32)).astype(BF16)
    return high, mid, low


def stack3(val):
    return jnp.concatenate(split3(val), axis=0)


def dot6(stack, b_high, b_mid, b_low, dims):
    rows = stack.shape[0] // 3
    o_high = lax.dot_general(stack, b_high, dims, preferred_element_type=F32)
    o_mid = lax.dot_general(stack[:2 * rows], b_mid, dims, preferred_element_type=F32)
    o_low = lax.dot_general(stack[:rows], b_low, dims, preferred_element_type=F32)
    small = (o_high[2 * rows:] + o_mid[rows:]) + o_low
    return o_high[:rows] + ((o_high[rows:2 * rows] + o_mid[:rows]) + small)


def v_table():
    table = {}

    def add(at, what, blk):
        table.setdefault((at // 4 - 1, at % 4), []).append((what, blk))

    for what, quarters in (('fwd', FWD), ('own', OWN), ('diag', DIAG), ('here', HERE)):
        for blk, at in enumerate(quarters):
            if at is not None:
                add(at, what, blk)
    return table


def kernel(v, tt, z4, o, vb, zb, vp, xt, stage, zst, tbv, ts, tp, ys, wsend, wrecv, gacc, gsend, grecv, osb,
           v_s, v_r, z_s, z_r, zl, tb_s, tb_r, tb_l, t_s, t_r, w_s, w_r, g_s, g_r, st_a, st_b, o_s, o_r, o_l):
    r = lax.axis_index('row')
    c = lax.axis_index('col')
    zz, yy, xx, kk = r // 2, r % 2, c // 2, c % 2
    dev_x = (r, (1 - xx) * 2 + kk)
    dev_y = (zz * 2 + (1 - yy), c)
    dev_z = ((1 - zz) * 2 + yy, c)
    dev_p = (r, xx * 2 + (1 - kk))
    dev_d = (zz * 2 + yy + (1 - kk) * (1 - 2 * yy), (xx + kk * (1 - 2 * xx)) * 2 + kk)

    barrier = pltpu.get_barrier_semaphore()
    for dev in (dev_x, dev_y, dev_z, dev_p):
        pl.semaphore_signal(barrier, 1, device_id=dev, device_id_type=MESH)
    pl.semaphore_wait(barrier, 4)

    def remote(src, dst, s_sem, r_sem, dev):
        return pltpu.make_async_remote_copy(src_ref=src, dst_ref=dst, send_sem=s_sem, recv_sem=r_sem,
                                            device_id=dev, device_id_type=MESH)

    def mult(val, by):
        return val if isinstance(val, int) else pl.multiple_of(val, by)

    def own(qq, idx, dev):
        r0 = 128 * qq
        return remote(v.at[pl.ds(r0, 2048 - r0), pl.ds(r0, 128)], vb.at[qq, idx, pl.ds(r0, 2048 - r0)],
                      v_s.at[qq, idx], v_r.at[qq, idx], dev)

    def fwd(qq, src, idx, dev):
        r0 = 128 * qq
        return remote(vb.at[qq, src, pl.ds(r0, 2048 - r0)], vb.at[qq, idx, pl.ds(r0, 2048 - r0)],
                      v_s.at[qq, idx], v_r.at[qq, idx], dev)

    def slab(qq, idx):
        if idx in (0, 1, 3):
            return own(qq, idx, {0: dev_p, 1: dev_x, 3: dev_y}[idx])
        if idx == 5:
            return fwd(qq, 1 + 2 * kk, 5, dev_d)
        return fwd(qq, idx - 1, idx, dev_p)

    def at_trip(i, table):
        for first in range(-1, NBLK, 4):
            mine = [t for t in range(first, first + 4) if t in table]
            if mine:
                @pl.when((i >= first) & (i < first + 4))
                def _():
                    for trip in mine:
                        @pl.when(i == trip)
                        def _():
                            table[trip]()

    def send_own(qq):
        for idx in (1, 3, 0):
            slab(qq, idx).start()

    def pass_on(qq):
        for idx in (1, 3):
            slab(qq, idx).wait_recv()
        for idx in (5, 2, 4):
            slab(qq, idx).start()

    def pass_diag(qq):
        slab(qq, 5).wait_recv()
        slab(qq, 6).start()

    def stage_loads(q, ch, buf):
        rows = pl.ds(mult(256 * ch, 256), 256)
        cols = pl.ds(mult(128 * q, 128), 128)
        return (pltpu.make_async_copy(v.at[rows, cols], stage.at[buf, 0], st_a.at[buf]),
                pltpu.make_async_copy(vb.at[q, :, rows], stage.at[buf, pl.ds(1, 7)], st_b.at[buf]))

    def all_here(qq):
        for idx in (0, 2, 4, 6):
            slab(qq, idx).wait_recv()
        for j in range(min(2, 8 - qq // 2)):
            for cp in stage_loads(qq, 7 - j, j):
                cp.start()

    do = {'own': send_own, 'fwd': pass_on, 'diag': pass_diag, 'here': all_here}

    def run_of(events):
        def run():
            for what, blk in events:
                do[what](15 - blk)
        return run

    def z_copy(ch, y1):
        rows = pl.ds(mult(256 * ch, 256), 256)
        return remote(z4.at[2 * (1 - zz) + y1, rows], zb.at[y1, rows], z_s.at[ch, y1], z_r.at[ch, y1], dev_z)

    def z_loads(ch):
        rows = pl.ds(pl.multiple_of(256 * ch, 256), 256)
        return (pltpu.make_async_copy(z4.at[pl.ds(2 * zz, 2), rows], zst.at[zz], zl.at[0]),
                pltpu.make_async_copy(zb.at[:, rows], zst.at[1 - zz], zl.at[1]))

    halves = ((12, 4), (0, 12))

    def t_copy(half, way):
        q0, nq = halves[half]
        part = pl.ds(q0, nq)
        src = tbv.at[2, part] if way == 2 else tt.at[part]
        return remote(src, tbv.at[way + 1, part], tb_s.at[half, way], tb_r.at[half, way],
                      dev_x if way == 1 else dev_p)

    def w_copy(s, par):
        return remote(wsend.at[s, par], wrecv.at[s, par], w_s.at[s, par], w_r.at[s, par], dev_z)

    def g_copy(slot):
        return remote(gsend.at[slot], grecv.at[slot], g_s.at[slot], g_r.at[slot], dev_z)

    def s_copy(slot):
        return remote(ts.at[slot, kk], ts.at[slot, kk], t_s.at[slot], t_r.at[slot], dev_p)

    own_t = pltpu.make_async_copy(tt, tbv.at[0], tb_l)
    own_t.start()
    send_own(15)
    for way in range(2):
        t_copy(0, way).start()
    for y1 in range(2):
        z_copy(7, y1).start()
    pass_on(15)
    for y1 in range(2):
        z_copy(6, y1).start()
    send_own(13)
    pass_diag(15)
    send_own(14)
    own_t.wait()
    all_here(15)

    lane = lax.broadcasted_iota(jnp.int32, (128, 128), 1)
    left = lane < 64
    left64 = left[:64]

    def prepare(qn, slot):
        cq = qn // 2
        n = 8 - cq
        gacc[...] = jnp.zeros((192, 256), F32)

        def take(j):
            ch = 7 - j
            buf = j % 2
            for cp in stage_loads(qn, ch, buf):
                cp.wait()

        def parts(j):
            ch = 7 - j
            buf = j % 2
            empty = (qn % 2 == 1) & (ch == cq)
            for y1 in range(2):
                dy = (y1 + yy) % 2
                for h in range(2):
                    for pair in range(2):
                        dx = (pair + xx) % 2
                        rel = dy * 4 + dx * 2
                        a0 = stage[buf, rel + kk, pl.ds(128 * h, 128), :]
                        a1 = stage[buf, rel + 1 - kk, pl.ds(128 * h, 128), :]
                        if h == 0:
                            a0 = jnp.where(empty, 0.0, a0)
                            a1 = jnp.where(empty, 0.0, a1)
                        swap = pltpu.roll(jnp.where(left, a1, a0), 64, 1)
                        vals = (jnp.where(left, a0, swap), jnp.where(left, swap, a1))
                        for par in range(2):
                            for piece, val in enumerate(split3(vals[par])):
                                vp[slot, par, piece, ch, pl.ds(y1 * 256 + h * 128, 128),
                                   pl.ds(pair * 128, 128)] = val

        def more_loads(j):
            @pl.when(j + 2 < n)
            def _():
                for cp in stage_loads(qn, 5 - j, j % 2):
                    cp.start()

        def gram(j):
            vh, vm, vl = (vp[slot, kk, piece, 7 - j] for piece in range(3))
            lhs = jnp.concatenate([vh.T[64:], vm.T[64:], vl.T[64:]], axis=0)
            prod = dot6(lhs, vh, vm, vl, NN)
            gacc[...] += prod

        take(0)
        parts(0)
        more_loads(0)

        def trip(j, _):
            take(j)
            gram(j - 1)
            parts(j)
            more_loads(j)
            return 0
        lax.fori_loop(1, n, trip, 0)
        gram(n - 1)
        gsend[slot, pl.ds(0, 192)] = gacc[:, pl.ds(0, 128)]
        gsend[slot, pl.ds(192, 64)] = gacc[pl.ds(128, 64), pl.ds(128, 128)]

    def form_t(qn, slot):
        zero = jnp.zeros((64, 128), F32)

        def panel(e):
            val = tbv[(e // 2 + xx) % 2 * 2 + (e % 2 + kk) % 2, qn]
            other = pltpu.roll(val, 64, 1)
            return (jnp.where(left64, jnp.where(kk == 0, val, other), 0.0),
                    jnp.where(left64, 0.0, jnp.where(kk == 0, other, val)))

        def padded(val):
            return split3(jnp.concatenate([val, zero], axis=0))

        gram = gsend[slot] + grecv[slot]
        first, second = [], []
        for pair in range(2):
            low, high = panel(2 * pair)[0], panel(2 * pair + 1)
            near = jnp.where(left64, gram[192 * pair:192 * pair + 64], 0.0)
            first.append(dot6(stack3(high[0]), *padded(near), NN))
            second.append((low, high[1]))
        pairs = []
        for pair in range(2):
            low, high = second[pair]
            pairs.append(jnp.concatenate([low, high - dot6(stack3(first[pair]), *padded(low), NN)], axis=0))
        far = dot6(stack3(pairs[1]), *split3(gram[64:192]), NN)
        far = dot6(stack3(far), *split3(pairs[0]), NN)
        ts[slot, kk, pl.ds(0, 128), pl.ds(0, 128)] = pairs[0]
        ts[slot, kk, pl.ds(0, 128), pl.ds(128, 128)] = jnp.zeros((128, 128), F32)
        ts[slot, kk, pl.ds(128, 128), pl.ds(0, 128)] = -far
        ts[slot, kk, pl.ds(128, 128), pl.ds(128, 128)] = pairs[1]

    def update(s, slot, par, ch):
        yst = ys[...]
        delta = dot6(yst, vp[slot, par, 0, ch], vp[slot, par, 1, ch], vp[slot, par, 2, ch], NT)
        new = xt[s, ch] - delta
        xt[s, ch] = new
        return new

    def project(s, slot, par, ch):
        return dot6(stack3(xt[s, ch]), vp[slot, par, 0, ch], vp[slot, par, 1, ch], vp[slot, par, 2, ch], NN)

    def out_copies(s, ch):
        rows = pl.ds(pl.multiple_of(256 * ch, 256), 256)
        cols = pl.ds(pl.multiple_of((2 * s + yy) * 128, 128), 128)
        return (pltpu.make_async_copy(osb.at[s, ch, yy], o.at[rows, cols], o_l.at[s, ch]),
                remote(osb.at[s, ch, 1 - yy], o.at[rows, cols], o_s.at[s, ch], o_r.at[s, ch], dev_y))

    events = v_table()

    def step(g, _):
        i = g // 4 - 1
        sub = g % 4
        q = 15 - i
        qn = 14 - i
        par = 1 - sub // 2
        s = sub % 2
        cur = (i + 2) % 2
        nxt = (i + 1) % 2
        more = i < 15

        for quarter in range(4):
            here = {trip: run_of(ev) for (trip, at), ev in events.items() if at == quarter}

            @pl.when(sub == quarter)
            def _():
                at_trip(i, here)

        @pl.when(g == 1)
        def _():
            t_copy(0, 1).wait_recv()
            t_copy(0, 2).start()

        @pl.when(g == 3)
        def _():
            t_copy(0, 0).wait_recv()
            t_copy(0, 2).wait_recv()

        @pl.when(g == 6)
        def _():
            t_copy(1, 0).start()
            t_copy(1, 1).start()

        @pl.when(g == 12)
        def _():
            t_copy(1, 1).wait_recv()
            t_copy(1, 2).start()

        @pl.when(g == 15)
        def _():
            t_copy(1, 0).wait_recv()
            t_copy(1, 2).wait_recv()

        @pl.when((sub == 0) & more)
        def _():
            prepare(qn, nxt)

        @pl.when((sub == 0) & (i >= 0))
        def _():
            s_copy(cur).wait()
            for pp in range(2):
                for piece, val in enumerate(split3(ts[cur, pp])):
                    tp[pp, piece] = val

        @pl.when((sub == 1) & more & (qn % 2 == 1))
        def _():
            ch = qn // 2
            for y1 in range(2):
                z_copy(ch, y1).wait_recv()
            for cp in z_loads(ch):
                cp.start()

        @pl.when((sub == 2) & more & (qn % 2 == 1))
        def _():
            ch = qn // 2
            for cp in z_loads(ch):
                cp.wait()
            for ss in range(2):
                for y1 in range(2):
                    xt[ss, ch, :, pl.ds(y1 * 256, 256)] = zst[ss, y1].T

        @pl.when((sub == 3) & more)
        def _():
            g_copy(nxt).wait()
            form_t(qn, nxt)
            s_copy(nxt).start()

        has_u = i >= 0
        has_w = ((i < 15) | (sub < 2)) & ((i >= 0) | (sub >= 2))
        n = 8 - q // 2
        w_par = 1 - par
        w_slot = jnp.where(sub < 2, cur, nxt)
        n_w = jnp.where(sub < 2, n, 8 - qn // 2)

        def solve():
            w_copy(s, par).wait()
            w_sum = wsend[s, par] + wrecv[s, par]
            ys[...] = stack3(dot6(stack3(w_sum), tp[par, 0], tp[par, 1], tp[par, 2], NN))

        for chunks in range(1, 9):
            @pl.when(has_u & has_w & (n == chunks))
            def _():
                solve()
                total = None
                for j in range(chunks + 1):
                    if j < chunks:
                        update(s, cur, par, 7 - j)
                    if j > 0:
                        prod = project(s, w_slot, w_par, 8 - j)
                        total = prod if total is None else total + prod
                wsend[s, w_par] = total

        @pl.when(has_w & jnp.logical_not(has_u))
        def _():
            wsend[s, w_par] = project(s, w_slot, w_par, 7)

        @pl.when(has_w & has_u & (n_w > n))
        def _():
            wsend[s, w_par] += project(s, w_slot, w_par, 7 - n)

        @pl.when(has_w)
        def _():
            w_copy(s, w_par).start()

        @pl.when((sub == 0) & more)
        def _():
            g_copy(nxt).start()

        @pl.when(((sub == 1) | (sub == 2)) & (qn % 2 == 1) & (qn >= 5))
        def _():
            z_copy(qn // 2 - 2, sub - 1).start()

        @pl.when(has_u & jnp.logical_not(has_w))
        def _():
            solve()
            update(s, cur, par, 7)

            def give(ch):
                for y1 in range(2):
                    osb[s, ch, y1] = xt[s, ch, :, pl.ds(y1 * 256, 256)].T
                for cp in out_copies(s, ch):
                    cp.start()

            def last(j, _):
                give(8 - j)
                update(s, cur, par, 7 - j)
                return 0
            lax.fori_loop(1, 8, last, 0)
            give(0)
        return 0

    lax.fori_loop(0, 4 * (NBLK + 1), step, 0)

    for half in range(2):
        for way in range(3):
            t_copy(half, way).wait_send()
    for qq in range(NBLK):
        for idx in range(7):
            slab(qq, idx).wait_send()

    def drain(ch, _):
        for y1 in range(2):
            z_copy(ch, y1).wait_send()
        for s in range(2):
            local, far = out_copies(s, ch)
            local.wait()
            far.wait()
        return 0
    lax.fori_loop(0, 8, drain, 0)


def solution(mesh):
    def local_apply(v_loc, t_loc, z_loc):
        tt = jnp.swapaxes(t_loc, 1, 2).reshape(NBLK, 2, 64, 64).transpose(0, 2, 1, 3).reshape(NBLK, 64, 128)
        z4 = z_loc.reshape(4, 2048, 128)
        any_spec = pl.BlockSpec(memory_space=pl.ANY)
        dma, vmem = pltpu.SemaphoreType.DMA, pltpu.VMEM
        out = pl.pallas_call(
            kernel,
            out_shape=(jax.ShapeDtypeStruct((2048, 512), F32),
                       jax.ShapeDtypeStruct((NBLK, 7, 2048, 128), F32),
                       jax.ShapeDtypeStruct((2, 2048, 128), F32)),
            in_specs=[any_spec] * 3,
            out_specs=(any_spec,) * 3,
            scratch_shapes=[
                vmem((2, 2, 3, 8, 512, 256), BF16),
                vmem((2, 8, 128, 512), F32),
                vmem((2, 8, 256, 128), F32),
                vmem((2, 2, 256, 128), F32),
                vmem((4, NBLK, 64, 128), F32),
                vmem((2, 2, 256, 256), F32),
                vmem((2, 3, 256, 256), BF16),
                vmem((384, 256), BF16),
                vmem((2, 2, 128, 256), F32),
                vmem((2, 2, 128, 256), F32),
                vmem((192, 256), F32),
                vmem((2, 256, 128), F32),
                vmem((2, 256, 128), F32),
                vmem((2, 8, 2, 256, 128), F32),
                dma((NBLK, 7)), dma((NBLK, 7)),
                dma((8, 2)), dma((8, 2)), dma((2,)),
                dma((2, 3)), dma((2, 3)), dma,
                dma((2,)), dma((2,)),
                dma((2, 2)), dma((2, 2)),
                dma((2,)), dma((2,)),
                dma((2,)), dma((2,)),
                dma((2, 8)), dma((2, 8)), dma((2, 8)),
            ],
            compiler_params=pltpu.CompilerParams(collective_id=0, has_side_effects=True, vmem_limit_bytes=64_000_000),
        )(v_loc, tt, z4)
        return out[0]

    return jax.shard_map(local_apply, mesh=mesh,
                         in_specs=(P('row', 'col'), P('col', None, None), P(None, ('col', 'row'))),
                         out_specs=P('row', 'col'), check_vma=False)
```

```python
import jax
import jax.numpy as jnp
from jax import lax
from jax.experimental import pallas as pl
from jax.experimental.pallas import tpu as pltpu
from jax.sharding import PartitionSpec as P

F32 = jnp.float32
BF16 = jnp.bfloat16
MESH = pl.DeviceIdType.MESH
NBLK = 16
REST = 0
OWN = (None, None, None, 4, 0, 4, 6, 9, 11, 20, 21, 21, 35, 36, 44, 51)
FWD = (None, 0, 3, 6, 6, 8, 19, 15, 17, 26, 32, 31, 40, 47, 49, 56)
DIAG = (None, 0, 4, 9, 9, 17, 23, 27, 29, 32, 36, 40, 46, 50, 53, 58)
HERE = (None, 3, 8, 11, 15, 19, 24, 28, 32, 36, 39, 43, 48, 51, 55, 59)
NT = (((1,), (1,)), ((), ()))
NN = (((1,), (0,)), ((), ()))


def split3(val):
    high = val.astype(BF16)
    rest = val - high.astype(F32)
    mid = rest.astype(BF16)
    low = (rest - mid.astype(F32)).astype(BF16)
    return high, mid, low


def stack3(val):
    return jnp.concatenate(split3(val), axis=0)


def dot6(stack, b_high, b_mid, b_low, dims):
    rows = stack.shape[0] // 3
    o_high = lax.dot_general(stack, b_high, dims, preferred_element_type=F32)
    o_mid = lax.dot_general(stack[:2 * rows], b_mid, dims, preferred_element_type=F32)
    o_low = lax.dot_general(stack[:rows], b_low, dims, preferred_element_type=F32)
    small = (o_high[2 * rows:] + o_mid[rows:]) + o_low
    return o_high[:rows] + ((o_high[rows:2 * rows] + o_mid[:rows]) + small)


def v_table():
    table = {}

    def add(at, what, blk):
        table.setdefault((at // 4 - 1, at % 4), []).append((what, blk))

    for what, quarters in (('fwd', FWD), ('own', OWN), ('diag', DIAG), ('here', HERE)):
        for blk, at in enumerate(quarters):
            if at is not None:
                add(at, what, blk)
    return table


def kernel(v, tt, z4, o, vb, zb, vp, xt, stage, zst, traw, tbv, ts, tp, ys, whalf, wsend, wrecv, gacc, gsend, grecv, osb, early, landed, y_out, y_in, yin,
           v_s, v_r, z_s, z_r, zl, tb_s, tb_r, tb_l, t_s, t_r, w_s, w_r, g_s, g_r, st_a, st_b, o_s, o_r, e_s, e_r, y_s, y_r):
    r = lax.axis_index('row')
    c = lax.axis_index('col')
    zz, yy, xx, kk = r // 2, r % 2, c // 2, c % 2
    dev_x = (r, (1 - xx) * 2 + kk)
    dev_y = (zz * 2 + (1 - yy), c)
    dev_z = ((1 - zz) * 2 + yy, c)
    dev_p = (r, xx * 2 + (1 - kk))
    dev_d = (zz * 2 + yy + (1 - kk) * (1 - 2 * yy), (xx + kk * (1 - 2 * xx)) * 2 + kk)

    barrier = pltpu.get_barrier_semaphore()
    for dev in (dev_x, dev_y, dev_z, dev_p):
        pl.semaphore_signal(barrier, 1, device_id=dev, device_id_type=MESH)
    pl.semaphore_wait(barrier, 4)

    def remote(src, dst, s_sem, r_sem, dev):
        return pltpu.make_async_remote_copy(src_ref=src, dst_ref=dst, send_sem=s_sem, recv_sem=r_sem,
                                            device_id=dev, device_id_type=MESH)

    def mult(val, by):
        return val if isinstance(val, int) else pl.multiple_of(val, by)

    def own(qq, idx, dev):
        r0 = 128 * qq
        return remote(v.at[pl.ds(r0, 2048 - r0), pl.ds(r0, 128)], vb.at[qq, idx, pl.ds(r0, 2048 - r0)],
                      v_s.at[qq, idx], v_r.at[qq, idx], dev)

    def fwd(qq, src, idx, dev):
        r0 = 128 * qq
        return remote(vb.at[qq, src, pl.ds(r0, 2048 - r0)], vb.at[qq, idx, pl.ds(r0, 2048 - r0)],
                      v_s.at[qq, idx], v_r.at[qq, idx], dev)

    def slab(qq, idx):
        if idx in (0, 1, 3):
            return own(qq, idx, {0: dev_p, 1: dev_x, 3: dev_y}[idx])
        if idx == 5:
            return fwd(qq, 1 + 2 * kk, 5, dev_d)
        return fwd(qq, idx - 1, idx, dev_p)

    def at_trip(i, table):
        for first in range(-1, NBLK, 4):
            mine = [t for t in range(first, first + 4) if t in table]
            if mine:
                @pl.when((i >= first) & (i < first + 4))
                def _():
                    for trip in mine:
                        @pl.when(i == trip)
                        def _():
                            table[trip]()

    def send_own(qq):
        for idx in (1, 3, 0):
            slab(qq, idx).start()

    def pass_on(qq):
        for idx in (1, 3):
            slab(qq, idx).wait_recv()
        for idx in (5, 2, 4):
            slab(qq, idx).start()

    def pass_diag(qq):
        slab(qq, 5).wait_recv()
        slab(qq, 6).start()

    def stage_loads(q, ch, buf):
        rows = pl.ds(mult(256 * ch, 256), 256)
        cols = pl.ds(mult(128 * q, 128), 128)
        return (pltpu.make_async_copy(v.at[rows, cols], stage.at[buf, 0], st_a.at[buf]),
                pltpu.make_async_copy(vb.at[q, :, rows], stage.at[buf, pl.ds(1, 7)], st_b.at[buf]))

    def all_here(qq):
        for idx in (0, 2, 4, 6):
            slab(qq, idx).wait_recv()
        for j in range(min(4, 8 - qq // 2)):
            for cp in stage_loads(qq, 7 - j, j):
                cp.start()

    do = {'own': send_own, 'fwd': pass_on, 'diag': pass_diag, 'here': all_here}

    def run_of(events):
        def run():
            for what, blk in events:
                do[what](15 - blk)
        return run

    def z_copy(ch, y1):
        rows = pl.ds(mult(256 * ch, 256), 256)
        return remote(z4.at[2 * (1 - zz) + y1, rows], zb.at[y1, rows], z_s.at[ch, y1], z_r.at[ch, y1], dev_z)

    def z_loads(ch):
        rows = pl.ds(pl.multiple_of(256 * ch, 256), 256)
        return (pltpu.make_async_copy(z4.at[pl.ds(2 * zz, 2), rows], zst.at[zz], zl.at[0]),
                pltpu.make_async_copy(zb.at[:, rows], zst.at[1 - zz], zl.at[1]))

    t_parts = ((12, 4), (0, 12))

    def t_copy(half, way):
        q0, nq = t_parts[half]
        part = pl.ds(q0, nq)
        src = tbv.at[2, part] if way == 2 else tbv.at[0, part]
        return remote(src, tbv.at[way + 1, part], tb_s.at[half, way], tb_r.at[half, way],
                      dev_x if way == 1 else dev_p)

    def w_copy(s, par):
        return remote(wsend.at[s, par], wrecv.at[s, par], w_s.at[s, par], w_r.at[s, par], dev_z)

    def g_copy(slot):
        return remote(gsend.at[slot], grecv.at[slot], g_s.at[slot], g_r.at[slot], dev_z)

    def s_copy(slot):
        return remote(ts.at[slot, kk], ts.at[slot, kk], t_s.at[slot], t_r.at[slot], dev_p)

    own_t = pltpu.make_async_copy(tt, traw, tb_l)
    own_t.start()
    send_own(15)
    own_t.wait()

    def pack(q, _):
        tbv[0, q] = jnp.concatenate([traw[2 * q], traw[2 * q + 1]], axis=0).T
        return 0
    lax.fori_loop(0, NBLK, pack, 0)
    for y1 in range(2):
        z_copy(6, y1).start()
    send_own(14)
    for y1 in range(2):
        z_copy(7, y1).start()
    pass_on(15)
    send_own(13)
    pass_diag(15)
    for way in range(2):
        t_copy(0, way).start()
    all_here(15)

    lane = lax.broadcasted_iota(jnp.int32, (128, 128), 1)
    left = lane < 64
    left64 = left[:64]

    def prepare(qn, slot):
        cq = qn // 2
        n = 8 - cq
        gacc[...] = jnp.zeros((192, 256), F32)

        def take(j):
            ch = 7 - j
            buf = j % 4
            for cp in stage_loads(qn, ch, buf):
                cp.wait()

        def parts(j):
            ch = 7 - j
            buf = j % 4
            empty = (qn % 2 == 1) & (ch == cq)
            for y1 in range(2):
                dy = (y1 + yy) % 2
                for h in range(2):
                    for pair in range(2):
                        dx = (pair + xx) % 2
                        rel = dy * 4 + dx * 2
                        a0 = stage[buf, rel + kk, pl.ds(128 * h, 128), :]
                        a1 = stage[buf, rel + 1 - kk, pl.ds(128 * h, 128), :]
                        if h == 0:
                            a0 = jnp.where(empty, 0.0, a0)
                            a1 = jnp.where(empty, 0.0, a1)
                        swap = pltpu.roll(jnp.where(left, a1, a0), 64, 1)
                        vals = (jnp.where(left, a0, swap), jnp.where(left, swap, a1))
                        for par in range(2):
                            for piece, val in enumerate(split3(vals[par])):
                                vp[slot, par, piece, ch, pl.ds(y1 * 256 + h * 128, 128),
                                   pl.ds(pair * 128, 128)] = val

        def more_loads(j):
            @pl.when(j + 4 < n)
            def _():
                for cp in stage_loads(qn, 3 - j, j % 4):
                    cp.start()

        def gram(j):
            vh, vm, vl = (vp[slot, kk, piece, 7 - j] for piece in range(3))
            lhs = jnp.concatenate([vh.T[64:], vm.T[64:], vl.T[64:]], axis=0)
            prod = dot6(lhs, vh, vm, vl, NN)
            gacc[...] += prod

        take(0)
        parts(0)
        more_loads(0)

        def trip(j, _):
            take(j)
            gram(j - 1)
            parts(j)
            more_loads(j)
            return 0
        lax.fori_loop(1, n, trip, 0)
        gram(n - 1)
        gsend[slot, pl.ds(0, 64)] = jnp.where(left64, gacc[pl.ds(0, 64), pl.ds(0, 128)],
                                              pltpu.roll(gacc[pl.ds(128, 64), pl.ds(128, 128)], 64, 1))
        gsend[slot, pl.ds(64, 128)] = gacc[pl.ds(64, 128), pl.ds(0, 128)]

    def form_t(qn, slot):
        zero = jnp.zeros((64, 128), F32)

        def panel(e):
            val = tbv[(e // 2 + xx) % 2 * 2 + (e % 2 + kk) % 2, qn]
            other = pltpu.roll(val, 64, 1)
            return (jnp.where(left64, jnp.where(kk == 0, val, other), 0.0),
                    jnp.where(left64, 0.0, jnp.where(kk == 0, other, val)))

        def padded(val):
            return split3(jnp.concatenate([val, zero], axis=0))

        gram = gsend[slot] + grecv[slot]
        first, second = [], []
        for pair in range(2):
            low, high = panel(2 * pair)[0], panel(2 * pair + 1)
            near = gram[:64] if pair == 0 else pltpu.roll(gram[:64], 64, 1)
            near = jnp.where(left64, near, 0.0)
            first.append(dot6(stack3(high[0]), *padded(near), NN))
            second.append((low, high[1]))
        pairs = []
        for pair in range(2):
            low, high = second[pair]
            pairs.append(jnp.concatenate([low, high - dot6(stack3(first[pair]), *padded(low), NN)], axis=0))
        far = dot6(stack3(pairs[1]), *split3(gram[64:192]), NN)
        far = dot6(stack3(far), *split3(pairs[0]), NN)
        ts[slot, kk, pl.ds(0, 128), pl.ds(0, 128)] = pairs[0]
        ts[slot, kk, pl.ds(0, 128), pl.ds(128, 128)] = jnp.zeros((128, 128), F32)
        ts[slot, kk, pl.ds(128, 128), pl.ds(0, 128)] = -far
        ts[slot, kk, pl.ds(128, 128), pl.ds(128, 128)] = pairs[1]

    def update(s, slot, par, ch):
        yst = ys[...]
        delta = dot6(yst, vp[slot, par, 0, ch], vp[slot, par, 1, ch], vp[slot, par, 2, ch], NT)
        new = xt[s, ch] - delta
        xt[s, ch] = new
        return new

    def project_half(s, slot, par, ch, t):
        part = pl.ds(256 * t, 256)
        return dot6(stack3(xt[s, ch, :, part]), *(vp[slot, par, piece, ch, part] for piece in range(3)), NN)

    def project(s, slot, par, ch):
        return dot6(stack3(xt[s, ch]), vp[slot, par, 0, ch], vp[slot, par, 1, ch], vp[slot, par, 2, ch], NN)

    near_half = pl.ds(pl.multiple_of(yy * 256, 256), 256)
    far_half = pl.ds(pl.multiple_of((1 - yy) * 256, 256), 256)

    def mult_rows(ch):
        return pl.ds(mult(256 * ch, 256), 256)

    def own_cols(s):
        return pl.ds(pl.multiple_of((2 * s + yy) * 128, 128), 128)

    def far_cols(s):
        return pl.ds(pl.multiple_of((2 * s + 1 - yy) * 128, 128), 128)

    def out_copy(ch):
        return remote(osb.at[ch], o.at[mult_rows(ch), own_cols(0)], o_s.at[ch], o_r.at[ch], dev_y)

    def early_copy():
        return remote(early, landed, e_s, e_r, dev_y)

    def y_copy(at):
        return remote(y_out.at[at], y_in.at[at], y_s.at[at], y_r.at[at], dev_y)

    events = v_table()

    def step(g, _):
        i = g // 4 - 1
        sub = g % 4
        q = 15 - i
        qn = 14 - i
        par = 1 - sub // 2
        s = sub % 2
        cur = (i + 2) % 2
        nxt = (i + 1) % 2
        more = i < 15

        for quarter in range(4):
            here = {trip: run_of(ev) for (trip, at), ev in events.items() if at == quarter}

            @pl.when(sub == quarter)
            def _():
                at_trip(i, here)

        @pl.when(g == 1)
        def _():
            t_copy(0, 1).wait_recv()
            t_copy(0, 2).start()

        @pl.when(g == 3)
        def _():
            t_copy(0, 0).wait_recv()
            t_copy(0, 2).wait_recv()

        @pl.when(g == REST)
        def _():
            t_copy(1, 0).start()
            t_copy(1, 1).start()

        @pl.when(g == REST + 6)
        def _():
            t_copy(1, 1).wait_recv()
            t_copy(1, 2).start()

        @pl.when(g == REST + 9)
        def _():
            t_copy(1, 0).wait_recv()
            t_copy(1, 2).wait_recv()

        @pl.when((sub == 0) & more)
        def _():
            prepare(qn, nxt)

        @pl.when((sub == 0) & (i >= 0))
        def _():
            s_copy(cur).wait()
            for pp in range(2):
                for piece, val in enumerate(split3(ts[cur, pp])):
                    tp[pp, piece] = val

        @pl.when((sub == 1) & more & (qn % 2 == 1))
        def _():
            ch = qn // 2
            for y1 in range(2):
                z_copy(ch, y1).wait_recv()
            for cp in z_loads(ch):
                cp.start()

        @pl.when((sub == 2) & more & (qn % 2 == 1))
        def _():
            ch = qn // 2
            for cp in z_loads(ch):
                cp.wait()
            for ss in range(2):
                for y1 in range(2):
                    xt[ss, ch, :, pl.ds(y1 * 256, 256)] = zst[ss, y1].T

        @pl.when((sub == 3) & more)
        def _():
            g_copy(nxt).wait()
            form_t(qn, nxt)
            s_copy(nxt).start()

        has_u = i >= 0
        has_w = ((i < 15) | (sub < 2)) & ((i >= 0) | (sub >= 2))
        n = 8 - q // 2
        w_par = 1 - par
        w_slot = jnp.where(sub < 2, cur, nxt)
        n_w = jnp.where(sub < 2, n, 8 - qn // 2)

        tell = (i >= NBLK - 2) & (s == 1)
        y_at = jnp.where(tell, 2 * (i - (NBLK - 2)) + 1 - par, 4)

        def solve():
            w_copy(s, par).wait()
            w_sum = wsend[s, par] + wrecv[s, par]
            halves = [dot6(stack3(w_sum[64 * h:64 * h + 64]), tp[par, 0], tp[par, 1], tp[par, 2], NN)
                      for h in range(2)]
            y_val = jnp.concatenate(halves, axis=0)
            ys[...] = stack3(y_val)
            y_out[y_at] = y_val

        for chunks in range(1, 9):
            @pl.when(has_u & has_w & (n == chunks))
            def _():
                solve()
                totals = [None, None]
                for j in range(chunks + 1):
                    if j < chunks:
                        update(s, cur, par, 7 - j)
                    if j > 0:
                        for t in range(2):
                            prod = project_half(s, w_slot, w_par, 8 - j, t)
                            totals[t] = prod if totals[t] is None else totals[t] + prod
                wsend[s, w_par] = totals[0]
                whalf[...] = totals[1]

        @pl.when(has_u & has_w)
        def _():
            wsend[s, w_par] += whalf[...]

        @pl.when(has_w & jnp.logical_not(has_u))
        def _():
            wsend[s, w_par] = project(s, w_slot, w_par, 7)

        @pl.when(has_w & has_u & (n_w > n))
        def _():
            wsend[s, w_par] += project(s, w_slot, w_par, 7 - n)

        @pl.when(has_w)
        def _():
            w_copy(s, w_par).start()

        @pl.when((sub == 0) & more)
        def _():
            g_copy(nxt).start()

        @pl.when(((sub == 1) | (sub == 2)) & (qn % 2 == 1) & (qn >= 5))
        def _():
            z_copy(qn // 2 - 2, sub - 1).start()

        @pl.when(tell & has_w)
        def _():
            y_copy(y_at).start()

        @pl.when((i == NBLK - 3) & (sub == 3))
        def _():
            def keep(ch, _):
                early[ch] = xt[1, ch, :, far_half]
                return 0
            lax.fori_loop(0, 8, keep, 0)
            early_copy().start()

        @pl.when((i == NBLK - 1) & (sub == 2))
        def _():
            solve()
            update(0, cur, 0, 7)

            def give(ch):
                osb[ch] = xt[0, ch, :, far_half].T
                out_copy(ch).start()
                o[mult_rows(ch), own_cols(0)] = xt[0, ch, :, near_half].T

            def last(j, _):
                give(8 - j)
                update(0, cur, 0, 7 - j)
                return 0
            lax.fori_loop(1, 8, last, 0)
            give(0)

        @pl.when((i == NBLK - 1) & (sub == 3))
        def _():
            solve()
            y_copy(3).start()

            def near(pair, _):
                yst = ys[...]
                for ch in (2 * pair, 2 * pair + 1):
                    delta = dot6(yst, *(vp[cur, 0, piece, ch, near_half] for piece in range(3)), NT)
                    o[mult_rows(ch), own_cols(1)] = (xt[1, ch, :, near_half] - delta).T
                return 0
            lax.fori_loop(0, 4, near, 0)

            early_copy().wait_recv()
            for at in range(4):
                y_copy(at).wait_recv()
                yin[at] = stack3(y_in[at])

            def far(pair, _):
                for ch in (2 * pair, 2 * pair + 1):
                    total = None
                    for at in range(4):
                        part = dot6(yin[at], *(vp[at // 2, 1 - at % 2, piece, ch, near_half] for piece in range(3)), NT)
                        total = part if total is None else total + part
                    o[mult_rows(ch), far_cols(1)] = (landed[ch] - total).T
                return 0
            lax.fori_loop(0, 4, far, 0)
        return 0

    lax.fori_loop(0, 4 * (NBLK + 1), step, 0)

    for half in range(2):
        for way in range(3):
            t_copy(half, way).wait_send()
    for qq in range(NBLK):
        for idx in range(7):
            slab(qq, idx).wait_send()

    early_copy().wait_send()
    for at in range(4):
        y_copy(at).wait_send()

    def drain(ch, _):
        for y1 in range(2):
            z_copy(ch, y1).wait_send()
        out_copy(ch).wait()
        return 0
    lax.fori_loop(0, 8, drain, 0)


def solution(mesh):
    def local_apply(v_loc, t_loc, z_loc):
        z4 = z_loc.reshape(4, 2048, 128)
        any_spec = pl.BlockSpec(memory_space=pl.ANY)
        dma, vmem = pltpu.SemaphoreType.DMA, pltpu.VMEM
        out = pl.pallas_call(
            kernel,
            out_shape=(pltpu.VMEM((2048, 512), F32),
                       jax.ShapeDtypeStruct((NBLK, 7, 2048, 128), F32),
                       jax.ShapeDtypeStruct((2, 2048, 128), F32)),
            in_specs=[any_spec] * 3,
            out_specs=(pl.BlockSpec(memory_space=pltpu.VMEM), any_spec, any_spec),
            scratch_shapes=[
                vmem((2, 2, 3, 8, 512, 256), BF16),
                vmem((2, 8, 128, 512), F32),
                vmem((4, 8, 256, 128), F32),
                vmem((2, 2, 256, 128), F32),
                vmem((32, 64, 64), F32),
                vmem((4, NBLK, 64, 128), F32),
                vmem((2, 2, 256, 256), F32),
                vmem((2, 3, 256, 256), BF16),
                vmem((384, 256), BF16),
                vmem((128, 256), F32),
                vmem((2, 2, 128, 256), F32),
                vmem((2, 2, 128, 256), F32),
                vmem((192, 256), F32),
                vmem((2, 192, 128), F32),
                vmem((2, 192, 128), F32),
                vmem((8, 256, 128), F32),
                vmem((8, 128, 256), F32),
                vmem((8, 128, 256), F32),
                vmem((5, 128, 256), F32),
                vmem((4, 128, 256), F32),
                vmem((4, 384, 256), BF16),
                dma((NBLK, 7)), dma((NBLK, 7)),
                dma((8, 2)), dma((8, 2)), dma((2,)),
                dma((2, 3)), dma((2, 3)), dma,
                dma((2,)), dma((2,)),
                dma((2, 2)), dma((2, 2)),
                dma((2,)), dma((2,)),
                dma((4,)), dma((4,)),
                dma((8,)), dma((8,)),
                dma, dma, dma((4,)), dma((4,)),
            ],
            compiler_params=pltpu.CompilerParams(collective_id=0, has_side_effects=True, vmem_limit_bytes=56_000_000),
        )(v_loc, t_loc, z4)
        return out[0]

    return jax.shard_map(local_apply, mesh=mesh,
                         in_specs=(P('row', 'col'), P('col', None, None), P(None, ('col', 'row'))),
                         out_specs=P('row', 'col'), check_vma=False)
```

```python
import jax
import jax.numpy as jnp
from jax import lax
from jax.experimental import pallas as pl
from jax.experimental.pallas import tpu as pltpu
from jax.sharding import PartitionSpec as P

F32 = jnp.float32
BF16 = jnp.bfloat16
MESH = pl.DeviceIdType.MESH
NBLK = 16
REST = 0
OWN = (None, None, None, 4, 0, 4, 6, 9, 11, 20, 21, 21, 35, 36, 44, 51)
FWD = (None, 0, 3, 6, 6, 8, 19, 15, 17, 26, 32, 31, 40, 47, 49, 56)
DIAG = (None, 0, 4, 9, 9, 17, 23, 27, 29, 32, 36, 40, 46, 50, 53, 58)
HERE = (None, 3, 8, 11, 15, 19, 24, 28, 32, 36, 39, 43, 48, 51, 55, 59)
NT = (((1,), (1,)), ((), ()))
NN = (((1,), (0,)), ((), ()))


def split3(val):
    high = val.astype(BF16)
    rest = val - high.astype(F32)
    mid = rest.astype(BF16)
    low = (rest - mid.astype(F32)).astype(BF16)
    return high, mid, low


def stack3(val):
    return jnp.concatenate(split3(val), axis=0)


def dot6(stack, b_high, b_mid, b_low, dims):
    rows = stack.shape[0] // 3
    o_high = lax.dot_general(stack, b_high, dims, preferred_element_type=F32)
    o_mid = lax.dot_general(stack[:2 * rows], b_mid, dims, preferred_element_type=F32)
    o_low = lax.dot_general(stack[:rows], b_low, dims, preferred_element_type=F32)
    small = (o_high[2 * rows:] + o_mid[rows:]) + o_low
    return o_high[:rows] + ((o_high[rows:2 * rows] + o_mid[:rows]) + small)


def v_table():
    table = {}

    def add(at, what, blk):
        table.setdefault((at // 4 - 1, at % 4), []).append((what, blk))

    for what, quarters in (('fwd', FWD), ('own', OWN), ('diag', DIAG), ('here', HERE)):
        for blk, at in enumerate(quarters):
            if at is not None:
                add(at, what, blk)
    return table


def kernel(v, tt, z4, o, vb, zb, vp, xt, stage, zst, traw, tbp, tbv, ts, tp, ys, whalf, wsend, wrecv, gacc, gsend, grecv, osb, early, landed, y_out, y_in, yin,
           v_s, v_r, z_s, z_r, zl, tb_s, tb_r, tb_l, t_s, t_r, w_s, w_r, g_s, g_r, st_a, st_b, o_s, o_r, e_s, e_r, y_s, y_r):
    r = lax.axis_index('row')
    c = lax.axis_index('col')
    zz, yy, xx, kk = r // 2, r % 2, c // 2, c % 2
    dev_x = (r, (1 - xx) * 2 + kk)
    dev_y = (zz * 2 + (1 - yy), c)
    dev_z = ((1 - zz) * 2 + yy, c)
    dev_p = (r, xx * 2 + (1 - kk))
    dev_d = (zz * 2 + yy + (1 - kk) * (1 - 2 * yy), (xx + kk * (1 - 2 * xx)) * 2 + kk)

    barrier = pltpu.get_barrier_semaphore()
    for dev in (dev_x, dev_y, dev_z, dev_p):
        pl.semaphore_signal(barrier, 1, device_id=dev, device_id_type=MESH)
    pl.semaphore_wait(barrier, 4)

    def remote(src, dst, s_sem, r_sem, dev):
        return pltpu.make_async_remote_copy(src_ref=src, dst_ref=dst, send_sem=s_sem, recv_sem=r_sem,
                                            device_id=dev, device_id_type=MESH)

    def mult(val, by):
        return val if isinstance(val, int) else pl.multiple_of(val, by)

    def is_short(dy, dx, dk):
        return 2 * zz + (yy + dy) % 2 < (xx + dx) % 2 * 2 + (kk + dk) % 2

    sent = [is_short(*at) for at in ((0, 0, 0), (0, 0, 0), (0, 1, 0), (0, 0, 0), (1, 0, 0), (kk, 1 - kk, 0), (1, 1, 0))]
    got = [is_short(*at) for at in ((0, 0, 1), (0, 1, 0), (0, 1, 1), (1, 0, 0), (1, 0, 1), (1, 1, 0), (1, 1, 1))]

    def slab(qq, idx, short):
        r0 = 128 * qq + (64 if short else 0)
        rows = pl.ds(r0, 2048 - r0)
        dev = {1: dev_x, 3: dev_y, 5: dev_d}.get(idx, dev_p)
        if idx in (0, 1, 3):
            src = v.at[rows, pl.ds(128 * qq, 128)]
        else:
            src = vb.at[qq, 1 + 2 * kk if idx == 5 else idx - 1, rows]
        return remote(src, vb.at[qq, idx, rows], v_s.at[qq, idx], v_r.at[qq, idx], dev)

    def send(qq, idx):
        for short in (True, False):
            @pl.when(sent[idx] == short)
            def _():
                slab(qq, idx, short).start()

    def receive(qq, idx):
        for short in (True, False):
            @pl.when(got[idx] == short)
            def _():
                slab(qq, idx, short).wait_recv()

    def at_trip(i, table):
        for first in range(-1, NBLK, 4):
            mine = [t for t in range(first, first + 4) if t in table]
            if mine:
                @pl.when((i >= first) & (i < first + 4))
                def _():
                    for trip in mine:
                        @pl.when(i == trip)
                        def _():
                            table[trip]()

    def send_own(qq):
        for idx in (1, 3, 0):
            send(qq, idx)

    def pass_on(qq):
        for idx in (1, 3):
            receive(qq, idx)
        for idx in (5, 2, 4):
            send(qq, idx)

    def pass_diag(qq):
        receive(qq, 5)
        send(qq, 6)

    def stage_loads(q, ch, buf):
        rows = pl.ds(mult(256 * ch, 256), 256)
        cols = pl.ds(mult(128 * q, 128), 128)
        return (pltpu.make_async_copy(v.at[rows, cols], stage.at[buf, 0], st_a.at[buf]),
                pltpu.make_async_copy(vb.at[q, :, rows], stage.at[buf, pl.ds(1, 7)], st_b.at[buf]))

    def all_here(qq):
        for idx in (0, 2, 4, 6):
            receive(qq, idx)
        for j in range(min(4, 8 - qq // 2)):
            for cp in stage_loads(qq, 7 - j, j):
                cp.start()

    do = {'own': send_own, 'fwd': pass_on, 'diag': pass_diag, 'here': all_here}

    def run_of(events):
        def run():
            for what, blk in events:
                do[what](15 - blk)
        return run

    def z_copy(ch, y1):
        rows = pl.ds(mult(256 * ch, 256), 256)
        return remote(z4.at[2 * (1 - zz) + y1, rows], zb.at[y1, rows], z_s.at[ch, y1], z_r.at[ch, y1], dev_z)

    def z_loads(ch):
        rows = pl.ds(pl.multiple_of(256 * ch, 256), 256)
        return (pltpu.make_async_copy(z4.at[pl.ds(2 * zz, 2), rows], zst.at[zz], zl.at[0]),
                pltpu.make_async_copy(zb.at[:, rows], zst.at[1 - zz], zl.at[1]))

    t_parts = ((6, 2), (0, 6))

    def t_copy(half, way):
        q0, nq = t_parts[half]
        part = pl.ds(q0, nq)
        src = tbp.at[2, part] if way == 2 else tbp.at[0, part]
        return remote(src, tbp.at[way + 1, part], tb_s.at[half, way], tb_r.at[half, way],
                      dev_x if way == 1 else dev_p)

    def w_copy(s, par):
        return remote(wsend.at[s, par], wrecv.at[s, par], w_s.at[s, par], w_r.at[s, par], dev_z)

    def g_copy(slot):
        return remote(gsend.at[slot], grecv.at[slot], g_s.at[slot], g_r.at[slot], dev_z)

    def s_copy(slot):
        return remote(ts.at[slot, kk], ts.at[slot, kk], t_s.at[slot], t_r.at[slot], dev_p)

    own_t = pltpu.make_async_copy(tt, traw, tb_l)
    own_t.start()
    send_own(15)
    own_t.wait()

    row64 = lax.broadcasted_iota(jnp.int32, (64, 128), 0)
    lane64 = lax.broadcasted_iota(jnp.int32, (64, 128), 1)

    def pack(pair, _):
        low = jnp.concatenate([traw[4 * pair], traw[4 * pair + 2]], axis=0).T
        high = jnp.concatenate([traw[4 * pair + 1].T, traw[4 * pair + 3].T], axis=0).T
        col = lane64 % 64
        tbp[0, pair, pl.ds(0, 64)] = jnp.where(row64 >= col, low, high)
        diag = jnp.sum(jnp.where(row64 == col, high, 0.0), axis=0, keepdims=True)
        tbp[0, pair, pl.ds(64, 8)] = jnp.broadcast_to(diag, (8, 128))
        return 0

    def unpack(at, _):
        q, src = at // 4, at % 4
        both = tbp[src, q // 2]
        both = jnp.where(q % 2 == 1, pltpu.roll(both, 64, 1), both)
        square, diag = both[:64], both[64:65]
        even = jnp.where((lane64 < 64) & (row64 >= lane64), square, 0.0)
        odd = jnp.where(row64 < lane64, square, jnp.where(row64 == lane64, jnp.broadcast_to(diag, (64, 128)), 0.0))
        odd = jnp.where(lane64 < 64, odd, 0.0)
        odd = jnp.concatenate([odd, jnp.zeros((64, 128), F32)], axis=0).T[:64]
        tbv[src, q] = jnp.where(kk == 0, even, odd)
        return 0

    lax.fori_loop(0, NBLK // 2, pack, 0)
    for y1 in range(2):
        z_copy(6, y1).start()
    send_own(14)
    for y1 in range(2):
        z_copy(7, y1).start()
    pass_on(15)
    send_own(13)
    pass_diag(15)
    for way in range(2):
        t_copy(0, way).start()
    all_here(15)

    lane = lax.broadcasted_iota(jnp.int32, (128, 128), 1)
    left = lane < 64
    left64 = left[:64]

    def part_of(slot, par, piece, ch, rows=slice(None)):
        return jnp.concatenate([vp[slot, par, piece, ch, side, rows] for side in range(2)], axis=1)

    def prepare(qn, slot):
        cq = qn // 2
        n = 8 - cq
        gacc[...] = jnp.zeros((192, 256), F32)

        def take(j):
            ch = 7 - j
            buf = j % 4
            for cp in stage_loads(qn, ch, buf):
                cp.wait()

            @pl.when(j == n - 1)
            def _():
                @pl.when(qn % 2 == 1)
                def _():
                    stage[buf, :, pl.ds(0, 128)] = jnp.zeros((8, 128, 128), F32)
                for rel in range(8):
                    @pl.when(is_short(rel // 4, rel // 2 % 2, rel % 2))
                    def _():
                        stage[buf, rel, pl.ds(pl.multiple_of(128 * (qn % 2), 128), 64)] = jnp.zeros((64, 128), F32)

        def parts(j):
            ch = 7 - j
            buf = j % 4
            for y1 in range(2):
                dy = (y1 + yy) % 2
                for h in range(2):
                    for pair in range(2):
                        dx = (pair + xx) % 2
                        rel = dy * 4 + dx * 2
                        a0 = stage[buf, rel + kk, pl.ds(128 * h, 128), :]
                        a1 = stage[buf, rel + 1 - kk, pl.ds(128 * h, 128), :]
                        swap = pltpu.roll(jnp.where(left, a1, a0), 64, 1)
                        vals = (jnp.where(left, a0, swap), jnp.where(left, swap, a1))
                        for par in range(2):
                            for piece, val in enumerate(split3(vals[par])):
                                vp[slot, par, piece, ch, pair, pl.ds(y1 * 256 + h * 128, 128)] = val

        def more_loads(j):
            @pl.when(j + 4 < n)
            def _():
                for cp in stage_loads(qn, 3 - j, j % 4):
                    cp.start()

        def gram(j):
            vh, vm, vl = (part_of(slot, kk, piece, 7 - j) for piece in range(3))
            lhs = jnp.concatenate([vh.T[64:], vm.T[64:], vl.T[64:]], axis=0)
            prod = dot6(lhs, vh, vm, vl, NN)
            gacc[...] += prod

        take(0)
        parts(0)
        more_loads(0)

        def trip(j, _):
            take(j)
            gram(j - 1)
            parts(j)
            more_loads(j)
            return 0
        lax.fori_loop(1, n, trip, 0)
        gram(n - 1)
        gsend[slot, pl.ds(0, 64)] = jnp.where(left64, gacc[pl.ds(0, 64), pl.ds(0, 128)],
                                              pltpu.roll(gacc[pl.ds(128, 64), pl.ds(128, 128)], 64, 1))
        gsend[slot, pl.ds(64, 128)] = gacc[pl.ds(64, 128), pl.ds(0, 128)]

    def form_t(qn, slot):
        zero = jnp.zeros((64, 128), F32)

        def panel(e):
            val = tbv[(e // 2 + xx) % 2 * 2 + (e % 2 + kk) % 2, qn]
            return val, pltpu.roll(val, 64, 1)

        def padded(val):
            return split3(jnp.concatenate([val, zero], axis=0))

        gram = gsend[slot] + grecv[slot]
        first, second = [], []
        for pair in range(2):
            low, high = panel(2 * pair)[0], panel(2 * pair + 1)
            near = gram[:64] if pair == 0 else pltpu.roll(gram[:64], 64, 1)
            near = jnp.where(left64, near, 0.0)
            first.append(dot6(stack3(high[0]), *padded(near), NN))
            second.append((low, high[1]))
        pairs = []
        for pair in range(2):
            low, high = second[pair]
            pairs.append(jnp.concatenate([low, high - dot6(stack3(first[pair]), *padded(low), NN)], axis=0))
        far = dot6(stack3(pairs[1]), *split3(gram[64:192]), NN)
        far = dot6(stack3(far), *split3(pairs[0]), NN)
        ts[slot, kk, pl.ds(0, 128), pl.ds(0, 128)] = pairs[0]
        ts[slot, kk, pl.ds(0, 128), pl.ds(128, 128)] = jnp.zeros((128, 128), F32)
        ts[slot, kk, pl.ds(128, 128), pl.ds(0, 128)] = -far
        ts[slot, kk, pl.ds(128, 128), pl.ds(128, 128)] = pairs[1]

    def update(s, slot, par, ch):
        yst = ys[...]
        delta = dot6(yst, *(part_of(slot, par, piece, ch) for piece in range(3)), NT)
        new = xt[s, ch] - delta
        xt[s, ch] = new
        return new

    def project_half(s, slot, par, ch, t):
        part = pl.ds(256 * t, 256)
        return dot6(stack3(xt[s, ch, :, part]), *(part_of(slot, par, piece, ch, part) for piece in range(3)), NN)

    def project(s, slot, par, ch):
        return dot6(stack3(xt[s, ch]), *(part_of(slot, par, piece, ch) for piece in range(3)), NN)

    near_half = pl.ds(pl.multiple_of(yy * 256, 256), 256)
    far_half = pl.ds(pl.multiple_of((1 - yy) * 256, 256), 256)

    def mult_rows(ch):
        return pl.ds(mult(256 * ch, 256), 256)

    def own_cols(s):
        return pl.ds(pl.multiple_of((2 * s + yy) * 128, 128), 128)

    def far_cols(s):
        return pl.ds(pl.multiple_of((2 * s + 1 - yy) * 128, 128), 128)

    def out_copy(ch):
        return remote(osb.at[ch], o.at[mult_rows(ch), own_cols(0)], o_s.at[ch], o_r.at[ch], dev_y)

    def early_copy():
        return remote(early, landed, e_s, e_r, dev_y)

    def y_copy(at):
        return remote(y_out.at[at], y_in.at[at], y_s.at[at], y_r.at[at], dev_y)

    events = v_table()

    def step(g, _):
        i = g // 4 - 1
        sub = g % 4
        q = 15 - i
        qn = 14 - i
        par = 1 - sub // 2
        s = sub % 2
        cur = (i + 2) % 2
        nxt = (i + 1) % 2
        more = i < 15

        for quarter in range(4):
            here = {trip: run_of(ev) for (trip, at), ev in events.items() if at == quarter}

            @pl.when(sub == quarter)
            def _():
                at_trip(i, here)

        @pl.when(g < REST + 10)
        def _():
            @pl.when(g == 1)
            def _():
                t_copy(0, 1).wait_recv()
                t_copy(0, 2).start()

            @pl.when(g == 3)
            def _():
                t_copy(0, 0).wait_recv()
                t_copy(0, 2).wait_recv()
                lax.fori_loop(48, 64, unpack, 0)

            @pl.when(g == REST)
            def _():
                t_copy(1, 0).start()
                t_copy(1, 1).start()

            @pl.when(g == REST + 6)
            def _():
                t_copy(1, 1).wait_recv()
                t_copy(1, 2).start()

            @pl.when(g == REST + 9)
            def _():
                t_copy(1, 0).wait_recv()
                t_copy(1, 2).wait_recv()
                lax.fori_loop(0, 48, unpack, 0)

        @pl.when((sub == 0) & more)
        def _():
            prepare(qn, nxt)

        @pl.when((sub == 0) & (i >= 0))
        def _():
            s_copy(cur).wait()
            for pp in range(2):
                for piece, val in enumerate(split3(ts[cur, pp])):
                    tp[pp, piece] = val

        @pl.when((sub == 1) & more & (qn % 2 == 1))
        def _():
            ch = qn // 2
            for y1 in range(2):
                z_copy(ch, y1).wait_recv()
            for cp in z_loads(ch):
                cp.start()

        @pl.when((sub == 2) & more & (qn % 2 == 1))
        def _():
            ch = qn // 2
            for cp in z_loads(ch):
                cp.wait()
            for ss in range(2):
                for y1 in range(2):
                    xt[ss, ch, :, pl.ds(y1 * 256, 256)] = zst[ss, y1].T

        @pl.when((sub == 3) & more)
        def _():
            g_copy(nxt).wait()
            form_t(qn, nxt)
            s_copy(nxt).start()

        has_u = i >= 0
        has_w = ((i < 15) | (sub < 2)) & ((i >= 0) | (sub >= 2))
        n = 8 - q // 2
        w_par = 1 - par
        w_slot = jnp.where(sub < 2, cur, nxt)
        n_w = jnp.where(sub < 2, n, 8 - qn // 2)

        tell = (i >= NBLK - 2) & (s == 1)
        y_at = jnp.where(tell, 2 * (i - (NBLK - 2)) + 1 - par, 4)

        def solve():
            w_copy(s, par).wait()
            w_sum = wsend[s, par] + wrecv[s, par]
            halves = [dot6(stack3(w_sum[64 * h:64 * h + 64]), tp[par, 0], tp[par, 1], tp[par, 2], NN)
                      for h in range(2)]
            y_val = jnp.concatenate(halves, axis=0)
            ys[...] = stack3(y_val)
            y_out[y_at] = y_val

        def both(chunks):
            solve()
            totals = [None, None]
            for j in range(chunks + 1):
                if j < chunks:
                    update(s, cur, par, 7 - j)
                if j > 0:
                    for t in range(2):
                        prod = project_half(s, w_slot, w_par, 8 - j, t)
                        totals[t] = prod if totals[t] is None else totals[t] + prod
            wsend[s, w_par] = totals[0]
            whalf[...] = totals[1]

        for first in range(1, 9, 4):
            @pl.when(has_u & has_w & (n >= first) & (n < first + 4))
            def _():
                for chunks in range(first, first + 4):
                    @pl.when(n == chunks)
                    def _():
                        both(chunks)

        @pl.when(has_w)
        def _():
            @pl.when(has_u)
            def _():
                wsend[s, w_par] += whalf[...]

                @pl.when(n_w > n)
                def _():
                    wsend[s, w_par] += project(s, w_slot, w_par, 7 - n)

            @pl.when(jnp.logical_not(has_u))
            def _():
                wsend[s, w_par] = project(s, w_slot, w_par, 7)
            w_copy(s, w_par).start()

        @pl.when((sub == 0) & more)
        def _():
            g_copy(nxt).start()

        @pl.when(((sub == 1) | (sub == 2)) & (qn % 2 == 1) & (qn >= 5))
        def _():
            z_copy(qn // 2 - 2, sub - 1).start()

        @pl.when(i >= NBLK - 3)
        def _():
            @pl.when(tell & has_w)
            def _():
                y_copy(y_at).start()

            @pl.when((i == NBLK - 3) & (sub == 3))
            def _():
                def keep(ch, _):
                    early[ch] = xt[1, ch, :, far_half]
                    return 0
                lax.fori_loop(0, 8, keep, 0)
                early_copy().start()

            @pl.when((i == NBLK - 1) & (sub == 2))
            def _():
                solve()
                update(0, cur, 0, 7)

                def give(ch):
                    osb[ch] = xt[0, ch, :, far_half].T

                    @pl.when(ch >= 6)
                    def _():
                        out_copy(ch).start()
                    o[mult_rows(ch), own_cols(0)] = xt[0, ch, :, near_half].T

                def last(j, _):
                    give(8 - j)
                    update(0, cur, 0, 7 - j)
                    return 0
                lax.fori_loop(1, 8, last, 0)
                osb[0] = xt[0, 0, :, far_half].T
                o[mult_rows(0), own_cols(0)] = xt[0, 0, :, near_half].T

            @pl.when((i == NBLK - 1) & (sub == 3))
            def _():
                solve()
                y_copy(3).start()
                for ch in range(5, -1, -1):
                    out_copy(ch).start()

                def near(pair, _):
                    yst = ys[...]
                    for ch in (2 * pair, 2 * pair + 1):
                        delta = dot6(yst, *(part_of(cur, 0, piece, ch, near_half) for piece in range(3)), NT)
                        o[mult_rows(ch), own_cols(1)] = (xt[1, ch, :, near_half] - delta).T
                    return 0
                lax.fori_loop(0, 4, near, 0)

                early_copy().wait_recv()
                for at in range(4):
                    y_copy(at).wait_recv()
                    yin[at] = stack3(y_in[at])

                def far(pair, _):
                    for ch in (2 * pair, 2 * pair + 1):
                        total = None
                        for at in range(4):
                            part = dot6(yin[at], *(part_of(at // 2, 1 - at % 2, piece, ch, near_half) for piece in range(3)), NT)
                            total = part if total is None else total + part
                        o[mult_rows(ch), far_cols(1)] = (landed[ch] - total).T
                    return 0
                lax.fori_loop(0, 4, far, 0)
        return 0

    lax.fori_loop(0, 4 * (NBLK + 1), step, 0)

    for half in range(2):
        for way in range(3):
            t_copy(half, way).wait_send()
    for qq in range(NBLK):
        for idx in range(7):
            for short in (True, False):
                @pl.when(sent[idx] == short)
                def _():
                    slab(qq, idx, short).wait_send()

    early_copy().wait_send()
    for at in range(4):
        y_copy(at).wait_send()

    def drain(ch, _):
        for y1 in range(2):
            z_copy(ch, y1).wait_send()
        out_copy(ch).wait()
        return 0
    lax.fori_loop(0, 8, drain, 0)


def solution(mesh):
    def local_apply(v_loc, t_loc, z_loc):
        z4 = z_loc.reshape(4, 2048, 128)
        any_spec = pl.BlockSpec(memory_space=pl.ANY)
        dma, vmem = pltpu.SemaphoreType.DMA, pltpu.VMEM
        out = pl.pallas_call(
            kernel,
            out_shape=(pltpu.VMEM((2048, 512), F32),
                       jax.ShapeDtypeStruct((NBLK, 7, 2048, 128), F32),
                       jax.ShapeDtypeStruct((2, 2048, 128), F32)),
            in_specs=[any_spec] * 3,
            out_specs=(pl.BlockSpec(memory_space=pltpu.VMEM), any_spec, any_spec),
            scratch_shapes=[
                vmem((2, 2, 3, 8, 2, 512, 128), BF16),
                vmem((2, 8, 128, 512), F32),
                vmem((4, 8, 256, 128), F32),
                vmem((2, 2, 256, 128), F32),
                vmem((32, 64, 64), F32),
                vmem((4, NBLK // 2, 72, 128), F32),
                vmem((4, NBLK, 64, 128), F32),
                vmem((2, 2, 256, 256), F32),
                vmem((2, 3, 256, 256), BF16),
                vmem((384, 256), BF16),
                vmem((128, 256), F32),
                vmem((2, 2, 128, 256), F32),
                vmem((2, 2, 128, 256), F32),
                vmem((192, 256), F32),
                vmem((2, 192, 128), F32),
                vmem((2, 192, 128), F32),
                vmem((8, 256, 128), F32),
                vmem((8, 128, 256), F32),
                vmem((8, 128, 256), F32),
                vmem((5, 128, 256), F32),
                vmem((4, 128, 256), F32),
                vmem((4, 384, 256), BF16),
                dma((NBLK, 7)), dma((NBLK, 7)),
                dma((8, 2)), dma((8, 2)), dma((2,)),
                dma((2, 3)), dma((2, 3)), dma,
                dma((2,)), dma((2,)),
                dma((2, 2)), dma((2, 2)),
                dma((2,)), dma((2,)),
                dma((4,)), dma((4,)),
                dma((8,)), dma((8,)),
                dma, dma, dma((4,)), dma((4,)),
            ],
            compiler_params=pltpu.CompilerParams(collective_id=0, has_side_effects=True, vmem_limit_bytes=56_000_000),
        )(v_loc, t_loc, z4)
        return out[0]

    return jax.shard_map(local_apply, mesh=mesh,
                         in_specs=(P('row', 'col'), P('col', None, None), P(None, ('col', 'row'))),
                         out_specs=P('row', 'col'), check_vma=False)
```

```python
import jax
import jax.numpy as jnp
from jax import lax
from jax.experimental import pallas as pl
from jax.experimental.pallas import tpu as pltpu
from jax.sharding import PartitionSpec as P

F32 = jnp.float32
BF16 = jnp.bfloat16
MESH = pl.DeviceIdType.MESH
EARLY = 5
NBLK = 16
REST = 7
OWN = (None, None, None, 2, 3, 0, 6, 13, 10, 23, 24, 20, 32, 39, 44, 52)
FWD = (None, 0, 0, 4, 6, 17, 12, 18, 17, 29, 33, 34, 37, 48, 50, 57)
DIAG = (None, 1, 6, 9, 12, 19, 18, 23, 25, 34, 38, 40, 44, 51, 53, 60)
HERE = (None, 2, 6, 11, 14, 20, 22, 27, 30, 35, 39, 43, 47, 52, 55, 60)
NT = (((1,), (1,)), ((), ()))
NN = (((1,), (0,)), ((), ()))


def split3(val):
    high = val.astype(BF16)
    rest = val - high.astype(F32)
    mid = rest.astype(BF16)
    low = (rest - mid.astype(F32)).astype(BF16)
    return high, mid, low


def stack3(val):
    return jnp.concatenate(split3(val), axis=0)


def dot6(stack, b_high, b_mid, b_low, dims, low_first=False):
    rows = stack.shape[0] // 3
    o_high = lax.dot_general(stack, b_high, dims, preferred_element_type=F32)
    if not low_first:
        o_mid = lax.dot_general(stack[:2 * rows], b_mid, dims, preferred_element_type=F32)
    o_low = lax.dot_general(stack[:rows], b_low, dims, preferred_element_type=F32)
    if low_first:
        o_mid = lax.dot_general(stack[:2 * rows], b_mid, dims, preferred_element_type=F32)
    small = (o_high[2 * rows:] + o_mid[rows:]) + o_low
    return o_high[:rows] + ((o_high[rows:2 * rows] + o_mid[:rows]) + small)


def v_table():
    table = {}

    def add(at, what, blk):
        table.setdefault((at // 4 - 1, at % 4), []).append((what, blk))

    for what, quarters in (('fwd', FWD), ('own', OWN), ('diag', DIAG), ('here', HERE)):
        for blk, at in enumerate(quarters):
            if at is not None:
                add(at, what, blk)
    return table


def kernel(v, tt, z4, o, vb, zb, vp, xt, stage, zst, traw, tbp, tbv, ts, tp, ys, whalf, wsend, wrecv, gacc, gsend, grecv, osb, early, landed, later, settled, y_out, y_in, yin,
           v_s, v_r, z_s, z_r, zl, tb_s, tb_r, tb_l, t_s, t_r, w_s, w_r, g_s, g_r, st_a, st_b, o_s, o_r, e_s, e_r, l_s, l_r, y_s, y_r):
    r = lax.axis_index('row')
    c = lax.axis_index('col')
    zz, yy, xx, kk = r // 2, r % 2, c // 2, c % 2
    dev_x = (r, (1 - xx) * 2 + kk)
    dev_y = (zz * 2 + (1 - yy), c)
    dev_z = ((1 - zz) * 2 + yy, c)
    dev_p = (r, xx * 2 + (1 - kk))
    dev_d = (zz * 2 + yy + (1 - kk) * (1 - 2 * yy), (xx + kk * (1 - 2 * xx)) * 2 + kk)

    barrier = pltpu.get_barrier_semaphore()
    for dev in (dev_x, dev_y, dev_z, dev_p):
        pl.semaphore_signal(barrier, 1, device_id=dev, device_id_type=MESH)
    pl.semaphore_wait(barrier, 4)

    def remote(src, dst, s_sem, r_sem, dev):
        return pltpu.make_async_remote_copy(src_ref=src, dst_ref=dst, send_sem=s_sem, recv_sem=r_sem,
                                            device_id=dev, device_id_type=MESH)

    def mult(val, by):
        return val if isinstance(val, int) else pl.multiple_of(val, by)

    def is_short(dy, dx, dk):
        return 2 * zz + (yy + dy) % 2 < (xx + dx) % 2 * 2 + (kk + dk) % 2

    sent = [is_short(*at) for at in ((0, 0, 0), (0, 0, 0), (0, 1, 0), (0, 0, 0), (1, 0, 0), (kk, 1 - kk, 0), (1, 1, 0))]
    got = [is_short(*at) for at in ((0, 0, 1), (0, 1, 0), (0, 1, 1), (1, 0, 0), (1, 0, 1), (1, 1, 0), (1, 1, 1))]

    def slab(qq, idx, short):
        r0 = 128 * qq + (64 if short else 0)
        rows = pl.ds(r0, 2048 - r0)
        dev = {1: dev_x, 3: dev_y, 5: dev_d}.get(idx, dev_p)
        if idx in (0, 1, 3):
            src = v.at[rows, pl.ds(128 * qq, 128)]
        else:
            src = vb.at[qq, 1 + 2 * kk if idx == 5 else idx - 1, rows]
        return remote(src, vb.at[qq, idx, rows], v_s.at[qq, idx], v_r.at[qq, idx], dev)

    def send(qq, idx):
        for short in (True, False):
            @pl.when(sent[idx] == short)
            def _():
                slab(qq, idx, short).start()

    def receive(qq, idx):
        for short in (True, False):
            @pl.when(got[idx] == short)
            def _():
                slab(qq, idx, short).wait_recv()

    def at_trip(i, table):
        for first in range(-1, NBLK, 4):
            mine = [t for t in range(first, first + 4) if t in table]
            if mine:
                @pl.when((i >= first) & (i < first + 4))
                def _():
                    for trip in mine:
                        @pl.when(i == trip)
                        def _():
                            table[trip]()

    def send_own(qq):
        for idx in (1, 3, 0):
            send(qq, idx)

    def pass_on(qq):
        for idx in (1, 3):
            receive(qq, idx)
        for idx in (5, 2, 4):
            send(qq, idx)

    def pass_diag(qq):
        receive(qq, 5)
        send(qq, 6)

    def stage_loads(q, ch, buf):
        rows = pl.ds(mult(256 * ch, 256), 256)
        cols = pl.ds(mult(128 * q, 128), 128)
        return (pltpu.make_async_copy(v.at[rows, cols], stage.at[buf, 0], st_a.at[buf]),
                pltpu.make_async_copy(vb.at[q, :, rows], stage.at[buf, pl.ds(1, 7)], st_b.at[buf]))

    def all_here(qq):
        for idx in (0, 2, 4, 6):
            receive(qq, idx)
        for j in range(min(4, 8 - qq // 2)):
            for cp in stage_loads(qq, 7 - j, j):
                cp.start()

    do = {'own': send_own, 'fwd': pass_on, 'diag': pass_diag, 'here': all_here}

    def run_of(events):
        def run():
            for what, blk in events:
                do[what](15 - blk)
        return run

    def z_copy(ch, y1):
        rows = pl.ds(mult(256 * ch, 256), 256)
        return remote(z4.at[2 * (1 - zz) + y1, rows], zb.at[y1, rows], z_s.at[ch, y1], z_r.at[ch, y1], dev_z)

    def z_loads(ch):
        rows = pl.ds(pl.multiple_of(256 * ch, 256), 256)
        return (pltpu.make_async_copy(z4.at[pl.ds(2 * zz, 2), rows], zst.at[zz], zl.at[0]),
                pltpu.make_async_copy(zb.at[:, rows], zst.at[1 - zz], zl.at[1]))

    t_parts = ((6, 2), (0, 6))

    def t_copy(half, way):
        q0, nq = t_parts[half]
        part = pl.ds(q0, nq)
        src = tbp.at[2, part] if way == 2 else tbp.at[0, part]
        return remote(src, tbp.at[way + 1, part], tb_s.at[half, way], tb_r.at[half, way],
                      dev_x if way == 1 else dev_p)

    def w_copy(s, par):
        return remote(wsend.at[s, par], wrecv.at[s, par], w_s.at[s, par], w_r.at[s, par], dev_z)

    def g_copy(slot):
        return remote(gsend.at[slot], grecv.at[slot], g_s.at[slot], g_r.at[slot], dev_z)

    def s_copy(slot):
        return remote(ts.at[slot, kk], ts.at[slot, kk], t_s.at[slot], t_r.at[slot], dev_p)

    own_t = pltpu.make_async_copy(tt, traw, tb_l)
    own_t.start()
    send_own(15)
    own_t.wait()

    row64 = lax.broadcasted_iota(jnp.int32, (64, 128), 0)
    lane64 = lax.broadcasted_iota(jnp.int32, (64, 128), 1)

    def pack(pair, _):
        low = jnp.concatenate([traw[4 * pair], traw[4 * pair + 2]], axis=0).T
        high = jnp.concatenate([traw[4 * pair + 1].T, traw[4 * pair + 3].T], axis=0).T
        col = lane64 % 64
        tbp[0, pair, pl.ds(0, 64)] = jnp.where(row64 >= col, low, high)
        diag = jnp.sum(jnp.where(row64 == col, high, 0.0), axis=0, keepdims=True)
        tbp[0, pair, pl.ds(64, 8)] = jnp.broadcast_to(diag, (8, 128))
        return 0

    def unpack(q, _):
        for src in range(4):
            both = tbp[src, q // 2]
            both = jnp.where(q % 2 == 1, pltpu.roll(both, 64, 1), both)
            square, diag = both[:64], both[64:65]
            even = jnp.where((lane64 < 64) & (row64 >= lane64), square, 0.0)
            odd = jnp.where(row64 < lane64, square, jnp.where(row64 == lane64, jnp.broadcast_to(diag, (64, 128)), 0.0))
            odd = jnp.where(lane64 < 64, odd, 0.0)
            odd = jnp.concatenate([odd, jnp.zeros((64, 128), F32)], axis=0).T[:64]
            tbv[src, q] = jnp.where(kk == 0, even, odd)
        return 0

    lax.fori_loop(0, NBLK // 2, pack, 0)
    for y1 in range(2):
        z_copy(6, y1).start()
    for y1 in range(2):
        z_copy(7, y1).start()
    send_own(14)
    pass_on(15)
    send_own(13)
    pass_diag(15)
    for way in range(2):
        t_copy(0, way).start()
    all_here(15)

    lane = lax.broadcasted_iota(jnp.int32, (128, 128), 1)
    left = lane < 64
    left64 = left[:64]

    def part_of(slot, par, piece, ch, rows=slice(None)):
        return jnp.concatenate([vp[slot, par, piece, ch, side, rows] for side in range(2)], axis=1)

    def prepare(qn, slot):
        cq = qn // 2
        n = 8 - cq
        gacc[...] = jnp.zeros((192, 256), F32)

        def take(j):
            ch = 7 - j
            buf = j % 4
            for cp in stage_loads(qn, ch, buf):
                cp.wait()

            @pl.when(j == n - 1)
            def _():
                @pl.when(qn % 2 == 1)
                def _():
                    stage[buf, :, pl.ds(0, 128)] = jnp.zeros((8, 128, 128), F32)
                for rel in range(8):
                    @pl.when(is_short(rel // 4, rel // 2 % 2, rel % 2))
                    def _():
                        stage[buf, rel, pl.ds(pl.multiple_of(128 * (qn % 2), 128), 64)] = jnp.zeros((64, 128), F32)

        def parts(j):
            ch = 7 - j
            buf = j % 4
            for y1 in range(2):
                dy = (y1 + yy) % 2
                for h in range(2):
                    for pair in range(2):
                        dx = (pair + xx) % 2
                        rel = dy * 4 + dx * 2
                        a0 = stage[buf, rel + kk, pl.ds(128 * h, 128), :]
                        a1 = stage[buf, rel + 1 - kk, pl.ds(128 * h, 128), :]
                        swap = pltpu.roll(jnp.where(left, a1, a0), 64, 1)
                        vals = (jnp.where(left, a0, swap), jnp.where(left, swap, a1))
                        for par in range(2):
                            for piece, val in enumerate(split3(vals[par])):
                                vp[slot, par, piece, ch, pair, pl.ds(y1 * 256 + h * 128, 128)] = val

        def more_loads(j):
            @pl.when(j + 4 < n)
            def _():
                for cp in stage_loads(qn, 3 - j, j % 4):
                    cp.start()

        def gram(j):
            vh, vm, vl = (part_of(slot, kk, piece, 7 - j) for piece in range(3))
            lhs = jnp.concatenate([vh.T[64:], vm.T[64:], vl.T[64:]], axis=0)
            prod = dot6(lhs, vh, vm, vl, NN)
            gacc[...] += prod

        take(0)
        parts(0)
        more_loads(0)

        def trip(j, _):
            take(j)
            gram(j - 1)
            parts(j)
            more_loads(j)
            return 0
        lax.fori_loop(1, n, trip, 0)
        gram(n - 1)
        gsend[slot, pl.ds(0, 64)] = jnp.where(left64, gacc[pl.ds(0, 64), pl.ds(0, 128)],
                                              pltpu.roll(gacc[pl.ds(128, 64), pl.ds(128, 128)], 64, 1))
        gsend[slot, pl.ds(64, 128)] = gacc[pl.ds(64, 128), pl.ds(0, 128)]

    def form_t(qn, slot):
        zero = jnp.zeros((64, 128), F32)

        def panel(e):
            val = tbv[(e // 2 + xx) % 2 * 2 + (e % 2 + kk) % 2, qn]
            return val, pltpu.roll(val, 64, 1)

        def padded(val):
            return split3(jnp.concatenate([val, zero], axis=0))

        gram = gsend[slot] + grecv[slot]
        first, second = [], []
        for pair in range(2):
            low, high = panel(2 * pair)[0], panel(2 * pair + 1)
            near = gram[:64] if pair == 0 else pltpu.roll(gram[:64], 64, 1)
            near = jnp.where(left64, near, 0.0)
            first.append(dot6(stack3(high[0]), *padded(near), NN))
            second.append((low, high[1]))
        pairs = []
        for pair in range(2):
            low, high = second[pair]
            pairs.append(jnp.concatenate([low, high - dot6(stack3(first[pair]), *padded(low), NN)], axis=0))
        far = dot6(stack3(pairs[1]), *split3(gram[64:192]), NN)
        far = dot6(stack3(far), *split3(pairs[0]), NN)
        ts[slot, kk, pl.ds(0, 128), pl.ds(0, 128)] = pairs[0]
        ts[slot, kk, pl.ds(0, 128), pl.ds(128, 128)] = jnp.zeros((128, 128), F32)
        ts[slot, kk, pl.ds(128, 128), pl.ds(0, 128)] = -far
        ts[slot, kk, pl.ds(128, 128), pl.ds(128, 128)] = pairs[1]

    def update(s, slot, par, ch):
        yst = ys[...]
        delta = dot6(yst, *(part_of(slot, par, piece, ch) for piece in range(3)), NT)
        new = xt[s, ch] - delta
        xt[s, ch] = new
        return new

    def project_half(s, slot, par, ch, t):
        part = pl.ds(256 * t, 256)
        return dot6(stack3(xt[s, ch, :, part]), *(part_of(slot, par, piece, ch, part) for piece in range(3)), NN, True)

    def project(s, slot, par, ch):
        return dot6(stack3(xt[s, ch]), *(part_of(slot, par, piece, ch) for piece in range(3)), NN)

    near_half = pl.ds(pl.multiple_of(yy * 256, 256), 256)
    far_half = pl.ds(pl.multiple_of((1 - yy) * 256, 256), 256)

    def mult_rows(ch):
        return pl.ds(mult(256 * ch, 256), 256)

    def own_cols(s):
        return pl.ds(pl.multiple_of((2 * s + yy) * 128, 128), 128)

    def far_cols(s):
        return pl.ds(pl.multiple_of((2 * s + 1 - yy) * 128, 128), 128)

    def out_copy(ch):
        return remote(osb.at[ch], o.at[mult_rows(ch), own_cols(0)], o_s.at[ch], o_r.at[ch], dev_y)

    def early_copy():
        return remote(early, landed, e_s, e_r, dev_y)

    def later_copy():
        return remote(later, settled, l_s, l_r, dev_y)

    def y_copy(at):
        return remote(y_out.at[at], y_in.at[at], y_s.at[at], y_r.at[at], dev_y)

    events = v_table()

    def step(g, _):
        i = g // 4 - 1
        sub = g % 4
        q = 15 - i
        qn = 14 - i
        par = 1 - sub // 2
        s = sub % 2
        cur = (i + 2) % 2
        nxt = (i + 1) % 2
        more = i < 15

        for quarter in range(4):
            here = {trip: run_of(ev) for (trip, at), ev in events.items() if at == quarter}

            @pl.when(sub == quarter)
            def _():
                at_trip(i, here)

        @pl.when(g < 15)
        def _():
            @pl.when(g == 1)
            def _():
                t_copy(0, 1).wait_recv()
                t_copy(0, 2).start()

            @pl.when(g == 3)
            def _():
                t_copy(0, 0).wait_recv()
                t_copy(0, 2).wait_recv()
                lax.fori_loop(12, 16, unpack, 0)

            @pl.when(g == REST)
            def _():
                t_copy(1, 0).start()
                t_copy(1, 1).start()

            @pl.when(g == REST + 6)
            def _():
                t_copy(1, 1).wait_recv()
                t_copy(1, 2).start()

            @pl.when(g == 14)
            def _():
                t_copy(1, 0).wait_recv()
                t_copy(1, 2).wait_recv()
                lax.fori_loop(0, 12, unpack, 0)

        @pl.when((sub == 0) & more)
        def _():
            prepare(qn, nxt)

        @pl.when((sub == 0) & (i >= 0))
        def _():
            s_copy(cur).wait()
            for pp in range(2):
                for piece, val in enumerate(split3(ts[cur, pp])):
                    tp[pp, piece] = val

        @pl.when((sub == 1) & more & (qn % 2 == 1))
        def _():
            ch = qn // 2
            for y1 in range(2):
                z_copy(ch, y1).wait_recv()
            for cp in z_loads(ch):
                cp.start()

        @pl.when((sub == 2) & more & (qn % 2 == 1))
        def _():
            ch = qn // 2
            for cp in z_loads(ch):
                cp.wait()
            for ss in range(2):
                for y1 in range(2):
                    xt[ss, ch, :, pl.ds(y1 * 256, 256)] = zst[ss, y1].T

        @pl.when((sub == 3) & more)
        def _():
            g_copy(nxt).wait()
            form_t(qn, nxt)
            s_copy(nxt).start()

        has_u = i >= 0
        has_w = ((i < 15) | (sub < 2)) & ((i >= 0) | (sub >= 2))
        n = 8 - q // 2
        w_par = 1 - par
        w_slot = jnp.where(sub < 2, cur, nxt)
        n_w = jnp.where(sub < 2, n, 8 - qn // 2)

        tell = ((i >= NBLK - 2) & (s == 1)) | ((i == NBLK - 1) & (s == 0))
        y_at = jnp.where(tell, jnp.where(s == 1, 2 * (i - (NBLK - 2)), 4) + 1 - par, 6)

        def solve():
            w_copy(s, par).wait()
            w_sum = wsend[s, par] + wrecv[s, par]
            halves = [dot6(stack3(w_sum[64 * h:64 * h + 64]), tp[par, 0], tp[par, 1], tp[par, 2], NN)
                      for h in range(2)]
            y_val = jnp.concatenate(halves, axis=0)
            ys[...] = stack3(y_val)
            y_out[y_at] = y_val

        def both(chunks):
            solve()
            totals = [None, None]
            for j in range(chunks + 1):
                if j < chunks:
                    update(s, cur, par, 7 - j)
                if j > 0:
                    for t in range(2):
                        prod = project_half(s, w_slot, w_par, 8 - j, t)
                        totals[t] = prod if totals[t] is None else totals[t] + prod
            wsend[s, w_par] = totals[0]
            whalf[...] = totals[1]

        for first in range(1, 9, 4):
            @pl.when(has_u & has_w & (n >= first) & (n < first + 4))
            def _():
                for chunks in range(first, first + 4):
                    @pl.when(n == chunks)
                    def _():
                        both(chunks)

        @pl.when(has_w)
        def _():
            @pl.when(has_u)
            def _():
                wsend[s, w_par] += whalf[...]

                @pl.when(n_w > n)
                def _():
                    wsend[s, w_par] += project(s, w_slot, w_par, 7 - n)

            @pl.when(jnp.logical_not(has_u))
            def _():
                wsend[s, w_par] = project(s, w_slot, w_par, 7)
            w_copy(s, w_par).start()

        @pl.when((sub == 0) & more)
        def _():
            g_copy(nxt).start()

        @pl.when(((sub == 1) | (sub == 2)) & (qn % 2 == 1) & (qn >= 5))
        def _():
            z_copy(qn // 2 - 2, sub - 1).start()

        @pl.when(i >= NBLK - 3)
        def _():
            @pl.when(tell & has_w)
            def _():
                y_copy(y_at).start()

            @pl.when((i == NBLK - 3) & (sub == 3))
            def _():
                def keep(ch, _):
                    early[ch] = xt[1, ch, :, far_half]
                    return 0
                lax.fori_loop(0, 8, keep, 0)
                early_copy().start()

            @pl.when((i == NBLK - 2) & (sub == 2))
            def _():
                def keep(ch, _):
                    later[ch - EARLY] = xt[0, ch, :, far_half]
                    return 0
                lax.fori_loop(EARLY, 8, keep, 0)
                later_copy().start()

            @pl.when((i == NBLK - 1) & (sub == 2))
            def _():
                solve()
                y_copy(5).start()
                update(0, cur, 0, 7)

                def give(ch):
                    @pl.when(ch < EARLY)
                    def _():
                        osb[ch] = xt[0, ch, :, far_half].T

                    @pl.when((ch < EARLY) & (ch >= EARLY - 2))
                    def _():
                        out_copy(ch).start()
                    o[mult_rows(ch), own_cols(0)] = xt[0, ch, :, near_half].T

                def last(j, _):
                    give(8 - j)
                    update(0, cur, 0, 7 - j)
                    return 0
                lax.fori_loop(1, 8, last, 0)
                osb[0] = xt[0, 0, :, far_half].T
                o[mult_rows(0), own_cols(0)] = xt[0, 0, :, near_half].T

            @pl.when((i == NBLK - 1) & (sub == 3))
            def _():
                solve()
                y_copy(3).start()
                for ch in range(EARLY - 3, -1, -1):
                    out_copy(ch).start()

                def near(pair, _):
                    yst = ys[...]
                    for ch in (2 * pair, 2 * pair + 1):
                        delta = dot6(yst, *(part_of(cur, 0, piece, ch, near_half) for piece in range(3)), NT)
                        o[mult_rows(ch), own_cols(1)] = (xt[1, ch, :, near_half] - delta).T
                    return 0
                lax.fori_loop(0, 4, near, 0)

                def from_y(ch, ats):
                    total = None
                    for at in ats:
                        blk, p1 = (at // 2, 1 - at % 2) if at < 4 else (1, 5 - at)
                        part = dot6(yin[at], *(part_of(blk, p1, piece, ch, near_half) for piece in range(3)), NT)
                        total = part if total is None else total + part
                    return total

                def take_y(at):
                    y_copy(at).wait_recv()
                    yin[at] = stack3(y_in[at])

                early_copy().wait_recv()
                for at in range(3):
                    take_y(at)

                def far(pair, _):
                    for ch in (2 * pair, 2 * pair + 1):
                        landed[ch] -= from_y(ch, (0, 1, 2))
                    return 0
                lax.fori_loop(0, 4, far, 0)

                later_copy().wait_recv()
                for at in (4, 5):
                    take_y(at)
                for ch in range(EARLY, 8):
                    o[mult_rows(ch), far_cols(0)] = (settled[ch - EARLY] - from_y(ch, (4, 5))).T
                take_y(3)

                def final(pair, _):
                    for ch in (2 * pair, 2 * pair + 1):
                        o[mult_rows(ch), far_cols(1)] = (landed[ch] - from_y(ch, (3,))).T
                    return 0
                lax.fori_loop(0, 4, final, 0)
        return 0

    lax.fori_loop(0, 4 * (NBLK + 1), step, 0)

    for half in range(2):
        for way in range(3):
            t_copy(half, way).wait_send()
    for qq in range(NBLK):
        for idx in range(7):
            for short in (True, False):
                @pl.when(sent[idx] == short)
                def _():
                    slab(qq, idx, short).wait_send()

    early_copy().wait_send()
    later_copy().wait_send()
    for at in range(6):
        y_copy(at).wait_send()

    def drain(ch, _):
        for y1 in range(2):
            z_copy(ch, y1).wait_send()
        return 0
    lax.fori_loop(0, 8, drain, 0)
    for ch in range(EARLY - 1, -1, -1):
        out_copy(ch).wait()


def solution(mesh):
    def local_apply(v_loc, t_loc, z_loc):
        z4 = z_loc.reshape(4, 2048, 128)
        any_spec = pl.BlockSpec(memory_space=pl.ANY)
        dma, vmem = pltpu.SemaphoreType.DMA, pltpu.VMEM
        out = pl.pallas_call(
            kernel,
            out_shape=(pltpu.VMEM((2048, 512), F32),
                       jax.ShapeDtypeStruct((NBLK, 7, 2048, 128), F32),
                       jax.ShapeDtypeStruct((2, 2048, 128), F32)),
            in_specs=[any_spec] * 3,
            out_specs=(pl.BlockSpec(memory_space=pltpu.VMEM), any_spec, any_spec),
            scratch_shapes=[
                vmem((2, 2, 3, 8, 2, 512, 128), BF16),
                vmem((2, 8, 128, 512), F32),
                vmem((4, 8, 256, 128), F32),
                vmem((2, 2, 256, 128), F32),
                vmem((32, 64, 64), F32),
                vmem((4, NBLK // 2, 72, 128), F32),
                vmem((4, NBLK, 64, 128), F32),
                vmem((2, 2, 256, 256), F32),
                vmem((2, 3, 256, 256), BF16),
                vmem((384, 256), BF16),
                vmem((128, 256), F32),
                vmem((2, 2, 128, 256), F32),
                vmem((2, 2, 128, 256), F32),
                vmem((192, 256), F32),
                vmem((2, 192, 128), F32),
                vmem((2, 192, 128), F32),
                vmem((8, 256, 128), F32),
                vmem((8, 128, 256), F32),
                vmem((8, 128, 256), F32),
                vmem((8 - EARLY, 128, 256), F32),
                vmem((8 - EARLY, 128, 256), F32),
                vmem((7, 128, 256), F32),
                vmem((6, 128, 256), F32),
                vmem((6, 384, 256), BF16),
                dma((NBLK, 7)), dma((NBLK, 7)),
                dma((8, 2)), dma((8, 2)), dma((2,)),
                dma((2, 3)), dma((2, 3)), dma,
                dma((2,)), dma((2,)),
                dma((2, 2)), dma((2, 2)),
                dma((2,)), dma((2,)),
                dma((4,)), dma((4,)),
                dma((8,)), dma((8,)),
                dma, dma, dma, dma,
                dma((6,)), dma((6,)),
            ],
            compiler_params=pltpu.CompilerParams(collective_id=0, has_side_effects=True, vmem_limit_bytes=56_000_000),
        )(v_loc, t_loc, z4)
        return out[0]

    return jax.shard_map(local_apply, mesh=mesh,
                         in_specs=(P('row', 'col'), P('col', None, None), P(None, ('col', 'row'))),
                         out_specs=P('row', 'col'), check_vma=False)
```

```python
import jax
import jax.numpy as jnp
from jax import lax
from jax.experimental import pallas as pl
from jax.experimental.pallas import tpu as pltpu
from jax.sharding import PartitionSpec as P

F32 = jnp.float32
BF16 = jnp.bfloat16
MESH = pl.DeviceIdType.MESH
EARLY = 5
NBLK = 16
REST = 6
OWN = (None, None, None, 1, 4, 5, 1, 7, 10, 20, 19, 27, 33, 40, 43, 52)
FWD = (None, 0, 5, 5, 6, 14, 16, 17, 24, 26, 27, 34, 38, 47, 50, 57)
DIAG = (None, 3, 6, 8, 13, 17, 19, 28, 29, 32, 37, 42, 45, 51, 53, 60)
HERE = (None, 3, 7, 10, 14, 20, 23, 28, 31, 34, 38, 43, 47, 52, 55, 60)
NT = (((1,), (1,)), ((), ()))
NN = (((1,), (0,)), ((), ()))


def split3(val):
    high = val.astype(BF16)
    rest = val - high.astype(F32)
    mid = rest.astype(BF16)
    low = (rest - mid.astype(F32)).astype(BF16)
    return high, mid, low


def stack3(val):
    return jnp.concatenate(split3(val), axis=0)


def dot6(stack, b_high, b_mid, b_low, dims, low_first=False):
    rows = stack.shape[0] // 3
    o_high = lax.dot_general(stack, b_high, dims, preferred_element_type=F32)
    if not low_first:
        o_mid = lax.dot_general(stack[:2 * rows], b_mid, dims, preferred_element_type=F32)
    o_low = lax.dot_general(stack[:rows], b_low, dims, preferred_element_type=F32)
    if low_first:
        o_mid = lax.dot_general(stack[:2 * rows], b_mid, dims, preferred_element_type=F32)
    small = (o_high[2 * rows:] + o_mid[rows:]) + o_low
    return o_high[:rows] + ((o_high[rows:2 * rows] + o_mid[:rows]) + small)


def v_table():
    table = {}

    def add(at, what, blk):
        table.setdefault((at // 4 - 1, at % 4), []).append((what, blk))

    for what, quarters in (('fwd', FWD), ('own', OWN), ('diag', DIAG), ('here', HERE)):
        for blk, at in enumerate(quarters):
            if at is not None:
                add(at, what, blk)
    return table


def kernel(v, tt, z4, o, vb, zb, vp, xt, stage, zst, traw, tbp, tbv, ts, tp, ys, whalf, wsend, wrecv, gacc, gsend, grecv, osb, early, landed, later, settled, y_out, y_in, yin,
           v_s, v_r, z_s, z_r, zl, tb_s, tb_r, tb_l, t_s, t_r, w_s, w_r, g_s, g_r, st_a, st_b, o_s, o_r, e_s, e_r, l_s, l_r, y_s, y_r):
    r = lax.axis_index('row')
    c = lax.axis_index('col')
    zz, yy, xx, kk = r // 2, r % 2, c // 2, c % 2
    dev_x = (r, (1 - xx) * 2 + kk)
    dev_y = (zz * 2 + (1 - yy), c)
    dev_z = ((1 - zz) * 2 + yy, c)
    dev_p = (r, xx * 2 + (1 - kk))
    dev_d = (zz * 2 + yy + (1 - kk) * (1 - 2 * yy), (xx + kk * (1 - 2 * xx)) * 2 + kk)

    barrier = pltpu.get_barrier_semaphore()
    for dev in (dev_x, dev_y, dev_z, dev_p):
        pl.semaphore_signal(barrier, 1, device_id=dev, device_id_type=MESH)
    pl.semaphore_wait(barrier, 4)

    def remote(src, dst, s_sem, r_sem, dev):
        return pltpu.make_async_remote_copy(src_ref=src, dst_ref=dst, send_sem=s_sem, recv_sem=r_sem,
                                            device_id=dev, device_id_type=MESH)

    def mult(val, by):
        return val if isinstance(val, int) else pl.multiple_of(val, by)

    def is_short(dy, dx, dk):
        return 2 * zz + (yy + dy) % 2 < (xx + dx) % 2 * 2 + (kk + dk) % 2

    sent = [is_short(*at) for at in ((0, 0, 0), (0, 0, 0), (0, 1, 0), (0, 0, 0), (1, 0, 0), (kk, 1 - kk, 0), (1, 1, 0))]
    got = [is_short(*at) for at in ((0, 0, 1), (0, 1, 0), (0, 1, 1), (1, 0, 0), (1, 0, 1), (1, 1, 0), (1, 1, 1))]

    def slab(qq, idx, short):
        r0 = 128 * qq + (64 if short else 0)
        rows = pl.ds(r0, 2048 - r0)
        dev = {1: dev_x, 3: dev_y, 5: dev_d}.get(idx, dev_p)
        if idx in (0, 1, 3):
            src = v.at[rows, pl.ds(128 * qq, 128)]
        else:
            src = vb.at[qq, 1 + 2 * kk if idx == 5 else idx - 1, rows]
        return remote(src, vb.at[qq, idx, rows], v_s.at[qq, idx], v_r.at[qq, idx], dev)

    def send(qq, idx):
        for short in (True, False):
            @pl.when(sent[idx] == short)
            def _():
                slab(qq, idx, short).start()

    def receive(qq, idx):
        for short in (True, False):
            @pl.when(got[idx] == short)
            def _():
                slab(qq, idx, short).wait_recv()

    def at_trip(i, table):
        for first in range(-1, NBLK, 4):
            mine = [t for t in range(first, first + 4) if t in table]
            if mine:
                @pl.when((i >= first) & (i < first + 4))
                def _():
                    for trip in mine:
                        @pl.when(i == trip)
                        def _():
                            table[trip]()

    def send_own(qq):
        for idx in (1, 3, 0):
            send(qq, idx)

    def pass_on(qq):
        for idx in (1, 3):
            receive(qq, idx)
        for idx in (5, 2, 4):
            send(qq, idx)

    def pass_diag(qq):
        receive(qq, 5)
        send(qq, 6)

    def stage_loads(q, ch, buf):
        rows = pl.ds(mult(256 * ch, 256), 256)
        cols = pl.ds(mult(128 * q, 128), 128)
        return (pltpu.make_async_copy(v.at[rows, cols], stage.at[buf, 0], st_a.at[buf]),
                pltpu.make_async_copy(vb.at[q, :, rows], stage.at[buf, pl.ds(1, 7)], st_b.at[buf]))

    def all_here(qq):
        for idx in (0, 2, 4, 6):
            receive(qq, idx)
        for j in range(min(4, 8 - qq // 2)):
            for cp in stage_loads(qq, 7 - j, j):
                cp.start()

    do = {'own': send_own, 'fwd': pass_on, 'diag': pass_diag, 'here': all_here}

    def run_of(events):
        def run():
            for what, blk in events:
                do[what](15 - blk)
        return run

    def z_copy(ch, y1):
        rows = pl.ds(mult(256 * ch, 256), 256)
        return remote(z4.at[2 * (1 - zz) + y1, rows], zb.at[y1, rows], z_s.at[ch, y1], z_r.at[ch, y1], dev_z)

    def z_loads(ch):
        rows = pl.ds(pl.multiple_of(256 * ch, 256), 256)
        return (pltpu.make_async_copy(z4.at[pl.ds(2 * zz, 2), rows], zst.at[zz], zl.at[0]),
                pltpu.make_async_copy(zb.at[:, rows], zst.at[1 - zz], zl.at[1]))

    t_parts = ((6, 2), (0, 6))

    def t_copy(half, way):
        q0, nq = t_parts[half]
        part = pl.ds(q0, nq)
        src = tbp.at[2, part] if way == 2 else tbp.at[0, part]
        return remote(src, tbp.at[way + 1, part], tb_s.at[half, way], tb_r.at[half, way],
                      dev_x if way == 1 else dev_p)

    def w_copy(s, par):
        return remote(wsend.at[s, par], wrecv.at[s, par], w_s.at[s, par], w_r.at[s, par], dev_z)

    def g_copy(slot):
        return remote(gsend.at[slot], grecv.at[slot], g_s.at[slot], g_r.at[slot], dev_z)

    def s_copy(slot):
        return remote(ts.at[slot, kk], ts.at[slot, kk], t_s.at[slot], t_r.at[slot], dev_p)

    own_t = pltpu.make_async_copy(tt, traw, tb_l)
    own_t.start()
    send_own(15)
    own_t.wait()

    row64 = lax.broadcasted_iota(jnp.int32, (64, 128), 0)
    lane64 = lax.broadcasted_iota(jnp.int32, (64, 128), 1)

    def pack(pair, _):
        low = jnp.concatenate([traw[4 * pair], traw[4 * pair + 2]], axis=0).T
        high = jnp.concatenate([traw[4 * pair + 1].T, traw[4 * pair + 3].T], axis=0).T
        col = lane64 % 64
        tbp[0, pair, pl.ds(0, 64)] = jnp.where(row64 >= col, low, high)
        diag = jnp.sum(jnp.where(row64 == col, high, 0.0), axis=0, keepdims=True)
        tbp[0, pair, pl.ds(64, 8)] = jnp.broadcast_to(diag, (8, 128))
        return 0

    def unpack(q, _):
        for src in range(4):
            both = tbp[src, q // 2]
            both = jnp.where(q % 2 == 1, pltpu.roll(both, 64, 1), both)
            square, diag = both[:64], both[64:65]
            even = jnp.where((lane64 < 64) & (row64 >= lane64), square, 0.0)
            odd = jnp.where(row64 < lane64, square, jnp.where(row64 == lane64, jnp.broadcast_to(diag, (64, 128)), 0.0))
            odd = jnp.where(lane64 < 64, odd, 0.0)
            odd = jnp.concatenate([odd, jnp.zeros((64, 128), F32)], axis=0).T[:64]
            tbv[src, q] = jnp.where(kk == 0, even, odd)
        return 0

    lax.fori_loop(0, NBLK // 2, pack, 0)
    for y1 in range(2):
        z_copy(7, y1).start()
    send_own(14)
    pass_on(15)
    send_own(13)
    for way in range(2):
        t_copy(0, way).start()
    pass_diag(15)
    all_here(15)
    for y1 in range(2):
        z_copy(6, y1).start()

    lane = lax.broadcasted_iota(jnp.int32, (128, 128), 1)
    left = lane < 64
    left64 = left[:64]

    def part_of(slot, par, piece, ch, rows=slice(None)):
        return jnp.concatenate([vp[slot, par, piece, ch, side, rows] for side in range(2)], axis=1)

    def prepare(qn, slot):
        cq = qn // 2
        n = 8 - cq
        gacc[...] = jnp.zeros((192, 256), F32)

        def take(j):
            ch = 7 - j
            buf = j % 4
            for cp in stage_loads(qn, ch, buf):
                cp.wait()

            @pl.when(j == n - 1)
            def _():
                @pl.when(qn % 2 == 1)
                def _():
                    stage[buf, :, pl.ds(0, 128)] = jnp.zeros((8, 128, 128), F32)
                for rel in range(8):
                    @pl.when(is_short(rel // 4, rel // 2 % 2, rel % 2))
                    def _():
                        stage[buf, rel, pl.ds(pl.multiple_of(128 * (qn % 2), 128), 64)] = jnp.zeros((64, 128), F32)

        def parts(j):
            ch = 7 - j
            buf = j % 4
            for y1 in range(2):
                dy = (y1 + yy) % 2
                for h in range(2):
                    for pair in range(2):
                        dx = (pair + xx) % 2
                        rel = dy * 4 + dx * 2
                        a0 = stage[buf, rel + kk, pl.ds(128 * h, 128), :]
                        a1 = stage[buf, rel + 1 - kk, pl.ds(128 * h, 128), :]
                        swap = pltpu.roll(jnp.where(left, a1, a0), 64, 1)
                        vals = (jnp.where(left, a0, swap), jnp.where(left, swap, a1))
                        for par in range(2):
                            for piece, val in enumerate(split3(vals[par])):
                                vp[slot, par, piece, ch, pair, pl.ds(y1 * 256 + h * 128, 128)] = val

        def more_loads(j):
            @pl.when(j + 4 < n)
            def _():
                for cp in stage_loads(qn, 3 - j, j % 4):
                    cp.start()

        def gram(j):
            vh, vm, vl = (part_of(slot, kk, piece, 7 - j) for piece in range(3))
            lhs = jnp.concatenate([vh.T[64:], vm.T[64:], vl.T[64:]], axis=0)
            prod = dot6(lhs, vh, vm, vl, NN)
            gacc[...] += prod

        take(0)
        parts(0)
        more_loads(0)

        def trip(j, _):
            take(j)
            gram(j - 1)
            parts(j)
            more_loads(j)
            return 0
        lax.fori_loop(1, n, trip, 0)
        gram(n - 1)
        gsend[slot, pl.ds(0, 64)] = jnp.where(left64, gacc[pl.ds(0, 64), pl.ds(0, 128)],
                                              pltpu.roll(gacc[pl.ds(128, 64), pl.ds(128, 128)], 64, 1))
        gsend[slot, pl.ds(64, 128)] = gacc[pl.ds(64, 128), pl.ds(0, 128)]

    def form_t(qn, slot):
        zero = jnp.zeros((64, 128), F32)

        def panel(e):
            val = tbv[(e // 2 + xx) % 2 * 2 + (e % 2 + kk) % 2, qn]
            return val, pltpu.roll(val, 64, 1)

        def padded(val):
            return split3(jnp.concatenate([val, zero], axis=0))

        gram = gsend[slot] + grecv[slot]
        first, second = [], []
        for pair in range(2):
            low, high = panel(2 * pair)[0], panel(2 * pair + 1)
            near = gram[:64] if pair == 0 else pltpu.roll(gram[:64], 64, 1)
            near = jnp.where(left64, near, 0.0)
            first.append(dot6(stack3(high[0]), *padded(near), NN))
            second.append((low, high[1]))
        pairs = []
        for pair in range(2):
            low, high = second[pair]
            pairs.append(jnp.concatenate([low, high - dot6(stack3(first[pair]), *padded(low), NN)], axis=0))
        far = dot6(stack3(pairs[1]), *split3(gram[64:192]), NN)
        far = dot6(stack3(far), *split3(pairs[0]), NN)
        ts[slot, kk, pl.ds(0, 128), pl.ds(0, 128)] = pairs[0]
        ts[slot, kk, pl.ds(0, 128), pl.ds(128, 128)] = jnp.zeros((128, 128), F32)
        ts[slot, kk, pl.ds(128, 128), pl.ds(0, 128)] = -far
        ts[slot, kk, pl.ds(128, 128), pl.ds(128, 128)] = pairs[1]

    def update(s, slot, par, ch):
        yst = ys[...]
        delta = dot6(yst, *(part_of(slot, par, piece, ch) for piece in range(3)), NT)
        new = xt[s, ch] - delta
        xt[s, ch] = new
        return new

    def project_half(s, slot, par, ch, t):
        part = pl.ds(256 * t, 256)
        return dot6(stack3(xt[s, ch, :, part]), *(part_of(slot, par, piece, ch, part) for piece in range(3)), NN, True)

    def project(s, slot, par, ch):
        return dot6(stack3(xt[s, ch]), *(part_of(slot, par, piece, ch) for piece in range(3)), NN)

    near_half = pl.ds(pl.multiple_of(yy * 256, 256), 256)
    far_half = pl.ds(pl.multiple_of((1 - yy) * 256, 256), 256)

    def mult_rows(ch):
        return pl.ds(mult(256 * ch, 256), 256)

    def own_cols(s):
        return pl.ds(pl.multiple_of((2 * s + yy) * 128, 128), 128)

    def far_cols(s):
        return pl.ds(pl.multiple_of((2 * s + 1 - yy) * 128, 128), 128)

    def out_copy(ch):
        return remote(osb.at[ch], o.at[mult_rows(ch), own_cols(0)], o_s.at[ch], o_r.at[ch], dev_y)

    def early_copy():
        return remote(early, landed, e_s, e_r, dev_y)

    def later_copy():
        return remote(later, settled, l_s, l_r, dev_y)

    def y_copy(at):
        return remote(y_out.at[at], y_in.at[at], y_s.at[at], y_r.at[at], dev_y)

    events = v_table()

    def step(g, _):
        i = g // 4 - 1
        sub = g % 4
        q = 15 - i
        qn = 14 - i
        par = 1 - sub // 2
        s = sub % 2
        cur = (i + 2) % 2
        nxt = (i + 1) % 2
        more = i < 15

        for quarter in range(4):
            here = {trip: run_of(ev) for (trip, at), ev in events.items() if at == quarter}

            @pl.when(sub == quarter)
            def _():
                at_trip(i, here)

        @pl.when(g < 15)
        def _():
            @pl.when(g == 1)
            def _():
                t_copy(0, 1).wait_recv()
                t_copy(0, 2).start()

            @pl.when(g == 3)
            def _():
                t_copy(0, 0).wait_recv()
                t_copy(0, 2).wait_recv()
                lax.fori_loop(12, 16, unpack, 0)

            @pl.when(g == REST)
            def _():
                t_copy(1, 0).start()
                t_copy(1, 1).start()

            @pl.when(g == REST + 6)
            def _():
                t_copy(1, 1).wait_recv()
                t_copy(1, 2).start()

            @pl.when(g == 14)
            def _():
                t_copy(1, 0).wait_recv()
                t_copy(1, 2).wait_recv()
                lax.fori_loop(0, 12, unpack, 0)

        @pl.when((sub == 0) & more)
        def _():
            prepare(qn, nxt)

        @pl.when((sub == 0) & (i >= 0))
        def _():
            s_copy(cur).wait()
            for pp in range(2):
                for piece, val in enumerate(split3(ts[cur, pp])):
                    tp[pp, piece] = val

        @pl.when((sub == 1) & more & (qn % 2 == 1))
        def _():
            ch = qn // 2
            for y1 in range(2):
                z_copy(ch, y1).wait_recv()
            for cp in z_loads(ch):
                cp.start()

        @pl.when((sub == 2) & more & (qn % 2 == 1))
        def _():
            ch = qn // 2
            for cp in z_loads(ch):
                cp.wait()
            for ss in range(2):
                for y1 in range(2):
                    xt[ss, ch, :, pl.ds(y1 * 256, 256)] = zst[ss, y1].T

        @pl.when((sub == 3) & more)
        def _():
            g_copy(nxt).wait()
            form_t(qn, nxt)
            s_copy(nxt).start()

        has_u = i >= 0
        has_w = ((i < 15) | (sub < 2)) & ((i >= 0) | (sub >= 2))
        n = 8 - q // 2
        w_par = 1 - par
        w_slot = jnp.where(sub < 2, cur, nxt)
        n_w = jnp.where(sub < 2, n, 8 - qn // 2)

        tell = ((i >= NBLK - 2) & (s == 1)) | ((i == NBLK - 1) & (s == 0))
        y_at = jnp.where(tell, jnp.where(s == 1, 2 * (i - (NBLK - 2)), 4) + 1 - par, 6)

        def solve():
            w_copy(s, par).wait()
            w_sum = wsend[s, par] + wrecv[s, par]
            halves = [dot6(stack3(w_sum[64 * h:64 * h + 64]), tp[par, 0], tp[par, 1], tp[par, 2], NN)
                      for h in range(2)]
            y_val = jnp.concatenate(halves, axis=0)
            ys[...] = stack3(y_val)
            y_out[y_at] = y_val

        def both(chunks):
            solve()
            totals = [None, None]
            for j in range(chunks + 1):
                if j < chunks:
                    update(s, cur, par, 7 - j)
                if j > 0:
                    for t in range(2):
                        prod = project_half(s, w_slot, w_par, 8 - j, t)
                        totals[t] = prod if totals[t] is None else totals[t] + prod
            wsend[s, w_par] = totals[0]
            whalf[...] = totals[1]

        for first in range(1, 9, 4):
            @pl.when(has_u & has_w & (n >= first) & (n < first + 4))
            def _():
                for chunks in range(first, first + 4):
                    @pl.when(n == chunks)
                    def _():
                        both(chunks)

        @pl.when(has_w)
        def _():
            @pl.when(has_u)
            def _():
                wsend[s, w_par] += whalf[...]

                @pl.when(n_w > n)
                def _():
                    wsend[s, w_par] += project(s, w_slot, w_par, 7 - n)

            @pl.when(jnp.logical_not(has_u))
            def _():
                wsend[s, w_par] = project(s, w_slot, w_par, 7)
            w_copy(s, w_par).start()

        @pl.when((sub == 0) & more)
        def _():
            g_copy(nxt).start()

        @pl.when(((sub == 1) | (sub == 2)) & (qn % 2 == 1) & (qn >= 5))
        def _():
            z_copy(qn // 2 - 2, sub - 1).start()

        @pl.when(i >= NBLK - 3)
        def _():
            @pl.when(tell & has_w)
            def _():
                y_copy(y_at).start()

            @pl.when((i == NBLK - 3) & (sub == 3))
            def _():
                def keep(ch, _):
                    early[ch] = xt[1, ch, :, far_half]
                    return 0
                lax.fori_loop(0, 8, keep, 0)
                early_copy().start()

            @pl.when((i == NBLK - 2) & (sub == 2))
            def _():
                def keep(ch, _):
                    later[ch - EARLY] = xt[0, ch, :, far_half]
                    return 0
                lax.fori_loop(EARLY, 8, keep, 0)
                later_copy().start()

            @pl.when((i == NBLK - 1) & (sub == 2))
            def _():
                solve()
                y_copy(5).start()
                update(0, cur, 0, 7)

                def give(ch):
                    @pl.when(ch < EARLY)
                    def _():
                        osb[ch] = xt[0, ch, :, far_half].T

                    @pl.when((ch < EARLY) & (ch >= EARLY - 2))
                    def _():
                        out_copy(ch).start()
                    o[mult_rows(ch), own_cols(0)] = xt[0, ch, :, near_half].T

                def last(j, _):
                    give(8 - j)
                    update(0, cur, 0, 7 - j)
                    return 0
                lax.fori_loop(1, 8, last, 0)
                osb[0] = xt[0, 0, :, far_half].T
                o[mult_rows(0), own_cols(0)] = xt[0, 0, :, near_half].T

            @pl.when((i == NBLK - 1) & (sub == 3))
            def _():
                solve()
                y_copy(3).start()
                for ch in range(EARLY - 3, -1, -1):
                    out_copy(ch).start()

                def near(pair, _):
                    yst = ys[...]
                    for ch in (2 * pair, 2 * pair + 1):
                        delta = dot6(yst, *(part_of(cur, 0, piece, ch, near_half) for piece in range(3)), NT)
                        o[mult_rows(ch), own_cols(1)] = (xt[1, ch, :, near_half] - delta).T
                    return 0
                lax.fori_loop(0, 4, near, 0)

                def from_y(ch, ats):
                    total = None
                    for at in ats:
                        blk, p1 = (at // 2, 1 - at % 2) if at < 4 else (1, 5 - at)
                        part = dot6(yin[at], *(part_of(blk, p1, piece, ch, near_half) for piece in range(3)), NT)
                        total = part if total is None else total + part
                    return total

                def take_y(at):
                    y_copy(at).wait_recv()
                    yin[at] = stack3(y_in[at])

                early_copy().wait_recv()
                for at in range(3):
                    take_y(at)

                def far(pair, _):
                    for ch in (2 * pair, 2 * pair + 1):
                        landed[ch] -= from_y(ch, (0, 1, 2))
                    return 0
                lax.fori_loop(0, 4, far, 0)

                later_copy().wait_recv()
                for at in (4, 5):
                    take_y(at)
                for ch in range(EARLY, 8):
                    o[mult_rows(ch), far_cols(0)] = (settled[ch - EARLY] - from_y(ch, (4, 5))).T
                take_y(3)

                def final(pair, _):
                    for ch in (2 * pair, 2 * pair + 1):
                        o[mult_rows(ch), far_cols(1)] = (landed[ch] - from_y(ch, (3,))).T
                    return 0
                lax.fori_loop(0, 4, final, 0)
        return 0

    lax.fori_loop(0, 4 * (NBLK + 1), step, 0)

    for half in range(2):
        for way in range(3):
            t_copy(half, way).wait_send()
    for qq in range(NBLK):
        for idx in range(7):
            for short in (True, False):
                @pl.when(sent[idx] == short)
                def _():
                    slab(qq, idx, short).wait_send()

    early_copy().wait_send()
    later_copy().wait_send()
    for at in range(6):
        y_copy(at).wait_send()

    def drain(ch, _):
        for y1 in range(2):
            z_copy(ch, y1).wait_send()
        return 0
    lax.fori_loop(0, 8, drain, 0)
    for ch in range(EARLY - 1, -1, -1):
        out_copy(ch).wait()


def solution(mesh):
    def local_apply(v_loc, t_loc, z_loc):
        z4 = z_loc.reshape(4, 2048, 128)
        any_spec = pl.BlockSpec(memory_space=pl.ANY)
        dma, vmem = pltpu.SemaphoreType.DMA, pltpu.VMEM
        out = pl.pallas_call(
            kernel,
            out_shape=(pltpu.VMEM((2048, 512), F32),
                       jax.ShapeDtypeStruct((NBLK, 7, 2048, 128), F32),
                       jax.ShapeDtypeStruct((2, 2048, 128), F32)),
            in_specs=[any_spec] * 3,
            out_specs=(pl.BlockSpec(memory_space=pltpu.VMEM), any_spec, any_spec),
            scratch_shapes=[
                vmem((2, 2, 3, 8, 2, 512, 128), BF16),
                vmem((2, 8, 128, 512), F32),
                vmem((4, 8, 256, 128), F32),
                vmem((2, 2, 256, 128), F32),
                vmem((32, 64, 64), F32),
                vmem((4, NBLK // 2, 72, 128), F32),
                vmem((4, NBLK, 64, 128), F32),
                vmem((2, 2, 256, 256), F32),
                vmem((2, 3, 256, 256), BF16),
                vmem((384, 256), BF16),
                vmem((128, 256), F32),
                vmem((2, 2, 128, 256), F32),
                vmem((2, 2, 128, 256), F32),
                vmem((192, 256), F32),
                vmem((2, 192, 128), F32),
                vmem((2, 192, 128), F32),
                vmem((8, 256, 128), F32),
                vmem((8, 128, 256), F32),
                vmem((8, 128, 256), F32),
                vmem((8 - EARLY, 128, 256), F32),
                vmem((8 - EARLY, 128, 256), F32),
                vmem((7, 128, 256), F32),
                vmem((6, 128, 256), F32),
                vmem((6, 384, 256), BF16),
                dma((NBLK, 7)), dma((NBLK, 7)),
                dma((8, 2)), dma((8, 2)), dma((2,)),
                dma((2, 3)), dma((2, 3)), dma,
                dma((2,)), dma((2,)),
                dma((2, 2)), dma((2, 2)),
                dma((2,)), dma((2,)),
                dma((4,)), dma((4,)),
                dma((8,)), dma((8,)),
                dma, dma, dma, dma,
                dma((6,)), dma((6,)),
            ],
            compiler_params=pltpu.CompilerParams(collective_id=0, has_side_effects=True, vmem_limit_bytes=56_000_000),
        )(v_loc, t_loc, z4)
        return out[0]

    return jax.shard_map(local_apply, mesh=mesh,
                         in_specs=(P('row', 'col'), P('col', None, None), P(None, ('col', 'row'))),
                         out_specs=P('row', 'col'), check_vma=False)
```
